32 devices in a mesh: rec: 8 (over z, y), vocab: 4 (over x, core).
Axes of the slice: x: 2, y: 2, z: 4, core: 2. Of those that a mesh axis runs over, the one named last changes fastest.
Arguments:
- features: bfloat16 [32, 192, 1280], P('rec'), may hold values from -1000 to 1000
- head_weight: bfloat16 [1280, 32768], P(None, ('vocab', 'rec')), may hold values from -0.15625 to 0.15625
- labels: int32 [32, 128], P('rec'), may hold values from 0 to 32767
- audio_len: int32 [32], P(('rec', 'vocab')), may hold values from 1 to 192, as said below
- transcript_len: int32 [32], P(('rec', 'vocab')), may hold values from 1 to 128
Outputs:
- label_logprob: float32 [32, 192, 128], P(('rec', 'vocab'))
- path_score: float32 [32], P(('rec', 'vocab'))
The draws below stay inside these ranges and needn't reach their ends.
Inputs may be any that keep to these rules, and one draw needn't show every extreme that they name: `audio_len`: each recording has at least as many frames in use as its transcript has labels.
All inputs are finite; a program needn't handle non-finite values.
Results may differ from the reference program's by a relative error of at most 0.00055.
Values may be sent and summed in bfloat16 or wider, within the bound.
A program may use at most 128 MiB of HBM per device.

```python
import math
import jax
import jax.numpy as jnp
import numpy as np
from jax import lax

D = 1280
VOCAB = 32768
FRAMES = 192
LABELS = 128
REC = 32


def draw_features(key, part):
    key_base = jax.random.fold_in(key, 0)
    values = jnp.clip(jax.random.normal(key_base, (REC, FRAMES, D), jnp.float32), -6.0, 6.0)
    values = values * 3.0
    return values.astype(jnp.bfloat16)


def length_pair(key):
    inner = jax.random.fold_in(key, 7)
    key_text, key_audio = jax.random.split(inner)
    text_len = jax.random.randint(key_text, (REC,), 1, LABELS + 1)
    text_len = text_len.at[1].set(LABELS)
    audio_len = jax.random.randint(key_audio, (REC,), text_len, FRAMES + 1)
    audio_len = jnp.maximum(audio_len, text_len)
    audio_len = audio_len.at[0].set(FRAMES)
    return (audio_len.astype(jnp.int32), text_len.astype(jnp.int32))


def draw_audio_len(key, part):
    return length_pair(key)[0]


def draw_transcript_len(key, part):
    return length_pair(key)[1]


def place_ends(array, rng, least, top_value):
    longest = array.shape.index(max(array.shape))
    spots = []
    for shift in (0, 1):
        where = [jax.random.randint(jax.random.fold_in(rng, axis), (), 0, length) for axis, length in enumerate(array.shape)]
        where[longest] = (where[longest] + shift) % array.shape[longest]
        spots.append(tuple(where))
    return array.at[spots[0]].set(least).at[spots[1]].set(top_value)


def block_levels(stream_key, dims, pieces, least, high):
    gain, own = 1.0, jax.random.fold_in(stream_key, 6)
    for axis_at, shards_of in pieces:
        steps = jnp.exp(jax.random.uniform(jax.random.fold_in(own, axis_at), (shards_of,), jnp.float32, least / len(pieces), high / len(pieces)))
        gain = gain * jnp.repeat(steps, dims[axis_at] // shards_of).reshape([-1 if axis == axis_at else 1 for axis in range(len(dims))])
    return gain


def cumulative_ranks(number_of, skew):
    portions = [(1 << 20) // math.isqrt(grade ** skew) + 1 for grade in range(1, number_of + 1)]
    deviation = 1 + sum(portions) // (1 << 30)
    return np.cumsum(np.array([max(1, weight // deviation) for weight in portions]))


def ranked_ids(rng, shape, amount, lean):
    grid = cumulative_ranks(amount, lean)
    lot = jax.random.randint(jax.random.fold_in(rng, 1), shape, 0, int(grid[amount - 1]))
    grade = jnp.searchsorted(jnp.asarray(grid, jnp.int32), lot, side="right")
    return jax.random.permutation(jax.random.fold_in(rng, 2), amount)[grade].astype(jnp.int32)


def normal_values(key, shape, width, reach, shards=(), dtype=jnp.bfloat16):
    drawn = jax.random.normal(key, shape, jnp.float32) * width
    if len(shards) > 0:
        drawn = block_levels(key, shape, shards, -0.22, 0.18) * drawn
    return jnp.clip(drawn, min=-reach, max=reach).astype(dtype)


def setup_inputs(seed: int = 0) -> dict:
    splits = jax.random.split(jax.random.key(seed), 6)
    return {
        "features": draw_features(jax.random.fold_in(splits[5], 71), 0),
        "head_weight": normal_values(splits[1], (D, VOCAB), D ** -0.5, 0.15625, ((1, 32),)),
        "labels": place_ends(ranked_ids(splits[2], (REC, LABELS), VOCAB, 2), jax.random.fold_in(splits[2], 3), 0, VOCAB - 1).astype(jnp.int32),
        "audio_len": draw_audio_len(jax.random.fold_in(splits[5], 71), 0),
        "transcript_len": draw_transcript_len(jax.random.fold_in(splits[5], 71), 0),
    }


negative_fill = -1e30


def viterbi(log_prob, audio_len, transcript_len):
    rec_count, frames, slots = log_prob.shape
    states = lax.iota(jnp.int32, slots)[None, :]
    target = states == (transcript_len[:, None] - 1)
    initial = jnp.where(states == 0, log_prob[:, 0, :], negative_fill)
    best_end = jnp.where(audio_len == 1, jnp.sum(jnp.where(target, initial, 0.0), 1), 0.0)

    def advance(frame_index, carry):
        current, best_end = carry
        shifted = jnp.concatenate([jnp.full_like(current[:, :1], negative_fill), current[:, :-1]], 1)
        emitted = lax.dynamic_index_in_dim(log_prob, frame_index, 1, keepdims=False)
        current = jnp.maximum(current, shifted) + emitted
        reached = jnp.sum(jnp.where(target, current, 0.0), 1)
        best_end = jnp.where(audio_len - 1 == frame_index, reached, best_end)
        return current, best_end

    current, best_end = lax.fori_loop(1, frames, advance, (initial, best_end))
    return best_end


def reference(features, head_weight, labels, audio_len, transcript_len):
    def per_recording(inputs):
        frame_feats, label_ids = inputs
        logits = jnp.dot(frame_feats, head_weight, preferred_element_type=jnp.float32)
        row_top = jnp.max(logits, 1)
        log_norm = row_top + jnp.log(jnp.sum(jnp.exp(logits - row_top[:, None]), 1))
        picked = jnp.take(logits.astype(jnp.bfloat16), label_ids, axis=1).astype(jnp.float32)
        return picked - log_norm[:, None]

    log_prob = lax.map(per_recording, (features, labels))
    return log_prob, viterbi(log_prob, audio_len, transcript_len)
```

```python
import functools
import jax
import jax.numpy as jnp
from jax import lax
from jax.experimental import pallas as pl
from jax.experimental.pallas import tpu as pltpu
from jax.sharding import PartitionSpec as P

MESH = pl.DeviceIdType.MESH
NEG = -1e30
LOW = -3e38
run = 6


def bits_of(size):
    bits = []
    bit = size // 2
    while bit >= 1:
        bits.append(bit)
        bit //= 2
    return bits


def flip(v, mask, size):
    for bit in bits_of(size):
        if mask & bit:
            v = v + bit * (1 - 2 * ((v // bit) % 2))
    return v


def emit_kernel(a, b, V, x, w, lab, pick, stat, xg, wg, lg, mx, sm, acc, sw, rw, sl, rl, sf, rf, sg, loc):
    r = lax.axis_index("rec")
    v = lax.axis_index("vocab")
    G = a * b
    m, k = r // a, r % a
    rec_dev, frames, width = x.shape
    own = rec_dev // V
    nc, cw = wg.shape[1], wg.shape[3]
    cols = nc * cw
    slots = lab.shape[2]
    half = V // 2
    bits = bits_of(V)
    col_peer = lambda d: (m * a + flip(k, d, a), v)
    row_peer = lambda d: (flip(m, d, b) * a + k, v)

    local = [pltpu.make_async_copy(x, xg.at[m], loc.at[0]), pltpu.make_async_copy(lab, lg.at[m], loc.at[1])]
    for c in range(nc):
        local.append(pltpu.make_async_copy(w.at[:, pl.ds(c * cw, cw)], wg.at[k, c], loc.at[2 + c]))
    for c in local:
        c.start()

    barrier = pltpu.get_barrier_semaphore()
    peers = [col_peer(d) for d in range(1, a)] + [row_peer(d) for d in range(1, b)]
    peers += [(r, flip(v, bit, V)) for bit in bits]
    for peer in peers:
        pl.semaphore_signal(barrier, inc=1, device_id=peer, device_id_type=MESH)
    pl.semaphore_wait(barrier, len(peers))
    for c in local:
        c.wait()

    def remote(ref, ss, rs, to):
        return pltpu.make_async_remote_copy(
            src_ref=ref, dst_ref=ref, send_sem=ss, recv_sem=rs, device_id=to, device_id_type=MESH
        )

    sent = []

    def launch(*args):
        c = remote(*args)
        c.start()
        sent.append(c)

    piece = lambda g, c: xg.at[g, pl.ds(c * own, own)]
    for d in range(1, b):
        launch(lg.at[m], sl.at[d - 1], rl.at[d - 1], row_peer(d))
    for c in range(nc):
        for d in range(1, a):
            launch(wg.at[k, c], sw.at[d - 1, c], rw.at[d - 1, c], col_peer(d))
    for d in range(1, b):
        launch(piece(m, v), sf.at[d - 1], rf.at[d - 1, 0], row_peer(d))

    used = [0]

    def arrive_piece(d, mask):
        low = (mask & -mask) if mask else V
        g = flip(m, d, b)
        src = piece(g, flip(v, mask, V))
        remote(src, sf.at[d - 1], rf.at[d - 1, mask], row_peer(d)).wait_recv()
        for bit in bits:
            if bit < low:
                launch(src, sg.at[used[0]], rf.at[d - 1, mask | bit], (r, flip(v, bit, V)))
                used[0] += 1

    def arrive_pair(p):
        d, h = order[p]
        if d == 0:
            return
        if h == 0:
            remote(lg.at[flip(m, d, b)], sl.at[d - 1], rl.at[d - 1], row_peer(d)).wait_recv()
        arrive_piece(d, 2 * h)
        arrive_piece(d, 2 * h + 1)

    def arrive_chunk(e):
        d, c = e // nc, e % nc
        if d:
            ref = wg.at[flip(k, d, a), c]
            remote(ref, sw.at[d - 1, c], rw.at[d - 1, c], col_peer(d)).wait_recv()

    unit = 2 * own
    rows = unit * frames
    order = [(d, h) for d in range(b) for h in range(half)]

    def place(d, h):
        return jnp.bitwise_xor(m, d), jnp.bitwise_xor(v // 2, h)

    def task(p, d, h, e):
        g, pr = place(d, h)
        ke = jnp.bitwise_xor(k, e // nc)
        c = e % nc
        xs = xg[g, pl.ds(pr * unit, unit)].reshape(rows, width)
        l = jnp.dot(xs, wg[ke, c], preferred_element_type=jnp.float32)
        old = mx[p]
        new = old
        for n in range(0, cw, 128):
            new = jnp.maximum(new, l[:, n : n + 128])
        s = sm[p] * jnp.exp(old - new)
        for n in range(0, cw, 128):
            s = s + jnp.exp(l[:, n : n + 128] - new)
        mx[p] = new
        sm[p] = s
        low = l.astype(jnp.bfloat16)
        base = (v * G + m * a + ke) * cols + c * cw
        ids = lax.broadcasted_iota(jnp.int32, (cw, slots), 0) + base
        for q in range(unit):
            hot = (ids == lg[g, pr * unit + q]).astype(jnp.float32).astype(jnp.bfloat16)
            got = jnp.dot(low[q * frames : (q + 1) * frames], hot, preferred_element_type=jnp.float32)
            acc[p, q] = acc[p, q] + got

    def clear(p, _):
        mx[p] = jnp.full((rows, 128), LOW, jnp.float32)
        sm[p] = jnp.zeros((rows, 128), jnp.float32)
        acc[p] = jnp.zeros((unit, frames, slots), jnp.float32)
        return 0

    pairs = b * half
    chunks = a * nc
    lax.fori_loop(0, pairs, clear, 0)

    when = []
    for p, (d, h) in enumerate(order):
        when.append((0.0 if d == 0 else 0.20 + 0.28 * (d - 1) + 0.18 * h, 0, p))
    for e in range(nc, chunks):
        when.append(((e - nc + 1) / nc, 1, e))
    when.sort()
    have_p, have_e = 0, nc

    for _, kind, i in when:
        if kind == 0:
            arrive_pair(i)
            d, h = order[i]
            lax.fori_loop(0, have_e, lambda e, _: (task(i, d, h, e), 0)[1], 0)
            have_p = i + 1
        else:
            arrive_chunk(i)
            lax.fori_loop(0, have_p, lambda p, _: (task(p, p // half, p % half, i), 0)[1], 0)
            have_e = i + 1

    lane = lax.broadcasted_iota(jnp.int32, (frames, 128), 1)

    def finish(p, _):
        g, pr = place(p // half, p % half)
        best = mx[p]
        top = jnp.max(best, 1, keepdims=True)
        total = jnp.sum(sm[p] * jnp.exp(best - top), 1, keepdims=True)
        for q in range(unit):
            at = g * rec_dev + pr * unit + q
            pick[at] = acc[p, q].astype(jnp.bfloat16)
            part = slice(q * frames, (q + 1) * frames)
            stat[at] = jnp.where(lane == 0, top[part], total[part]).T[:8]
        return 0

    lax.fori_loop(0, pairs, finish, 0)
    for c in sent:
        c.wait_send()


def exchange_kernel(a, b, V, pick, stat, po, so, pin, sin, pout, sout, sp1, rp1, ss1, rs1, sp, rp, ss, rs):
    r = lax.axis_index("rec")
    v = lax.axis_index("vocab")
    m, k = r // a, r % a
    half = V // 2
    side = v % 2
    me = m * half + v // 2
    n = b * half
    sibling = (r, flip(v, 1, V))
    peer = lambda d: (((me + d) % n) // half * a + k, ((me + d) % n) % half * 2 + side)
    barrier = pltpu.get_barrier_semaphore()
    for to in [sibling] + [peer(d) for d in range(1, n)]:
        pl.semaphore_signal(barrier, inc=1, device_id=to, device_id_type=MESH)
    pl.semaphore_wait(barrier, n)

    def remote(src, dst, s, t, to):
        return pltpu.make_async_remote_copy(
            src_ref=src, dst_ref=dst, send_sem=s, recv_sem=t, device_id=to, device_id_type=MESH
        )

    copies = []
    for e in range(n):
        copies.append(remote(pick.at[e, 1 - side], pin.at[e], sp1.at[e], rp1.at[e], sibling))
        copies.append(remote(stat.at[e, 1 - side], sin.at[e], ss1.at[e], rs1.at[e], sibling))
    for c in copies:
        c.start()
    row = lax.broadcasted_iota(jnp.int32, sin.shape[1:], 1)
    for e in range(n):
        copies[2 * e].wait_recv()
        copies[2 * e + 1].wait_recv()
        pout[e] = pick[e, side] + pin[e]
        mine, other = stat[e, side], sin[e]
        top = jnp.maximum(mine[:, 0:1], other[:, 0:1])
        total = mine * jnp.exp(mine[:, 0:1] - top) + other * jnp.exp(other[:, 0:1] - top)
        sout[e] = jnp.where(row == 0, top, total)
    for d in range(1, n):
        to = (me + d) % n
        for src, dst, s, t in ((pout, po, sp, rp), (sout, so, ss, rs)):
            c = remote(src.at[to], dst.at[me], s.at[d - 1], t.at[d - 1], peer(d))
            c.start()
            copies.append(c)
    po[me] = pout[me]
    so[me] = sout[me]
    for d in range(1, n):
        fr = (me + n - d) % n
        for src, dst, s, t in ((pout, po, sp, rp), (sout, so, ss, rs)):
            remote(src.at[fr], dst.at[fr], s.at[d - 1], t.at[d - 1], peer(d)).wait_recv()
    for c in copies:
        c.wait_send()


def align_kernel(alen, tlen, pick, stat, lp_ref, out_ref):
    n, own, frames, slots = pick.shape
    lane = lax.broadcasted_iota(jnp.int32, (1, slots), 1)
    for q in range(own):
        top = stat[0, q, 0:1, :]
        for i in range(1, n):
            top = jnp.maximum(top, stat[i, q, 0:1, :])
        total = jnp.zeros_like(top)
        for i in range(n):
            total = total + stat[i, q, 1:2, :] * jnp.exp(stat[i, q, 0:1, :] - top)
        norm = top + jnp.log(total)
        got = pick[0, q].astype(jnp.float32)
        for i in range(1, n):
            got = got + pick[i, q].astype(jnp.float32)
        lp_ref[q] = got - jnp.broadcast_to(norm, (slots, frames)).T
        last = alen[q] - 1
        first = jnp.where(lane == 0, lp_ref[q, 0:1, :], NEG)

        def block(t, steps, cur, best):
            emit = [lp_ref[q, pl.ds(t + i, 1), :] for i in range(steps)]
            rolled = [[e if c == 0 else pltpu.roll(e, c, 1) for c in range(steps - i)] for i, e in enumerate(emit)]
            moved = [cur] + [jnp.where(lane < c, NEG, pltpu.roll(cur, c, 1)) for c in range(1, steps + 1)]
            for i in range(steps):
                moved = [jnp.maximum(moved[c], moved[c + 1]) + rolled[i][c] for c in range(steps - i)]
                best = jnp.where(last == t + i, moved[0], best)
            return moved[0], best

        whole = (frames - 1) // run
        cur, best = lax.fori_loop(0, whole, lambda i, c: block(1 + i * run, run, *c), (first, first))
        if (frames - 1) % run:
            best = block(1 + whole * run, (frames - 1) % run, cur, best)[1]
        score = jnp.sum(jnp.where(lane == tlen[q] - 1, best, 0.0), 1, keepdims=True)
        out_ref[q] = jnp.broadcast_to(score, (8, 128))


def body(features, head_weight, labels, audio_len, transcript_len):
    rec_dev, frames, width = features.shape
    cols = head_weight.shape[1]
    slots = labels.shape[1]
    G, V = lax.axis_size("rec"), lax.axis_size("vocab")
    best = None
    a = 2
    while a < G:
        cost = (a - 1) * width * cols + (G // a - 1) * features.size
        if G % a == 0 and (best is None or cost < best[0]):
            best = (cost, a)
        a *= 2
    a = best[1]
    b = G // a
    own = rec_dev // V
    vmem = pl.BlockSpec(memory_space=pltpu.VMEM)
    hbm = pl.BlockSpec(memory_space=pl.ANY)
    smem = pl.BlockSpec(memory_space=pltpu.SMEM)
    dma = pltpu.SemaphoreType.DMA
    cw = min(256, cols)
    nc = cols // cw
    total = b * rec_dev
    unit = 2 * own
    pairs = b * (V // 2)
    rows = unit * frames
    pick, stat = pl.pallas_call(
        functools.partial(emit_kernel, a, b, V),
        out_shape=(
            jax.ShapeDtypeStruct((total, frames, slots), jnp.bfloat16),
            jax.ShapeDtypeStruct((total, 8, frames), jnp.float32),
        ),
        in_specs=[hbm] * 3,
        out_specs=(vmem, vmem),
        scratch_shapes=[
            pltpu.VMEM((b,) + features.shape, features.dtype),
            pltpu.VMEM((a, nc, width, cw), head_weight.dtype),
            pltpu.VMEM((b, rec_dev, 1, slots), jnp.int32),
            pltpu.VMEM((pairs, rows, 128), jnp.float32),
            pltpu.VMEM((pairs, rows, 128), jnp.float32),
            pltpu.VMEM((pairs, unit, frames, slots), jnp.float32),
            dma((a - 1, nc)), dma((a - 1, nc)), dma((b - 1,)), dma((b - 1,)),
            dma((b - 1,)), dma((b - 1, V)), dma(((b - 1) * (V - 1),)), dma((2 + nc,)),
        ],
        compiler_params=pltpu.CompilerParams(
            collective_id=0, has_side_effects=True, vmem_limit_bytes=60 * 1024 * 1024
        ),
        name="emit",
    )(features, head_weight, labels.reshape(rec_dev, 1, slots))

    n = b * (V // 2)
    pick = pick.reshape(n, 2, own, frames, slots)
    stat = stat.reshape(n, 2, own, 8, frames)
    picked = (n, own, frames, slots)
    stats = (n, own, 8, frames)
    po, so = pl.pallas_call(
        functools.partial(exchange_kernel, a, b, V),
        out_shape=(
            jax.ShapeDtypeStruct(picked, pick.dtype),
            jax.ShapeDtypeStruct(stats, stat.dtype),
        ),
        in_specs=[vmem] * 2,
        out_specs=(vmem, vmem),
        scratch_shapes=[pltpu.VMEM(picked, pick.dtype), pltpu.VMEM(stats, stat.dtype)] * 2
        + [dma((n,))] * 4
        + [dma((n - 1,))] * 4,
        compiler_params=pltpu.CompilerParams(collective_id=1, has_side_effects=True),
        name="exchange",
    )(pick, stat)

    log_prob, score = pl.pallas_call(
        align_kernel,
        out_shape=(
            jax.ShapeDtypeStruct((own, frames, slots), jnp.float32),
            jax.ShapeDtypeStruct((own, 8, 128), jnp.float32),
        ),
        in_specs=[smem, smem, vmem, vmem],
        out_specs=(vmem, vmem),
        name="align",
    )(audio_len, transcript_len, po, so)
    return log_prob, score[:, 0, 0]


def solution(mesh):
    return jax.shard_map(
        body,
        mesh=mesh,
        in_specs=(
            P("rec", None, None),
            P(None, ("vocab", "rec")),
            P("rec", None),
            P(("rec", "vocab")),
            P(("rec", "vocab")),
        ),
        out_specs=(P(("rec", "vocab"), None, None), P(("rec", "vocab"))),
        check_vma=False,
    )
```

```python
import functools
import jax
import jax.numpy as jnp
from jax import lax
from jax.experimental import pallas as pl
from jax.experimental.pallas import tpu as pltpu
from jax.sharding import PartitionSpec as P

MESH = pl.DeviceIdType.MESH
NEG = -1e30
LOW = -3e38
run = 6


def bits_of(size):
    bits = []
    bit = size // 2
    while bit >= 1:
        bits.append(bit)
        bit //= 2
    return bits


def flip(v, mask, size):
    for bit in bits_of(size):
        if mask & bit:
            v = v + bit * (1 - 2 * ((v // bit) % 2))
    return v


def emit_kernel(
    a, b, V, x, w, lab, pick_ref, stat_ref, xg, wg, lg, mx, sm, acc, logit,
    pp, pin, cs, xin, xout, zin, st, sin, cst, xst, zsrc, zst,
    sw, rw, sl, rl, su, sx, rf, sp, rp, ss, rs, sq, rq, sv, rv, sz, rz, sy, ry, loc,
):
    r = lax.axis_index("rec")
    v = lax.axis_index("vocab")
    G = a * b
    m, k = r // a, r % a
    rec_dev, frames, width = x.shape
    own = rec_dev // V
    nc, cw = wg.shape[1], wg.shape[3]
    cols = nc * cw
    slots = lab.shape[2]
    half = V // 2
    side = v % 2
    bits = bits_of(V)
    unit = 2 * own
    rows = unit * frames
    pairs = b * half
    chunks = a * nc

    def among(values, i):
        out = values[0]
        for j in range(1, len(values)):
            out = jnp.where(i == j, values[j], out)
        return out

    near = [sorted(range(b), key=lambda o: (abs(o - i), o)) for i in range(b)]
    turns = [among([near[i][t] ^ i for i in range(b)], m) for t in range(b)]
    turn = lambda t: turns[t] if isinstance(t, int) else among(turns, t)
    inner = (m > 0) & (m < b - 1)

    col_peer = lambda d: (m * a + flip(k, d, a), v)
    row_peer = lambda d: (flip(m, d, b) * a + k, v)
    line = lambda at: (at * a + k, v)
    sibling = (r, flip(v, 1, V))
    across = lambda h: (r, flip(v, 2 * h, V))

    local = [pltpu.make_async_copy(x, xg.at[m], loc.at[0]), pltpu.make_async_copy(lab, lg.at[m], loc.at[1])]
    for c in range(nc):
        local.append(pltpu.make_async_copy(w.at[:, pl.ds(c * cw, cw)], wg.at[k, c], loc.at[2 + c]))
    for c in local:
        c.start()

    barrier = pltpu.get_barrier_semaphore()
    peers = [col_peer(d) for d in range(1, a)] + [row_peer(d) for d in range(1, b)]
    peers += [(r, flip(v, mask, V)) for mask in sorted(set(bits + [2 * h for h in range(1, half)]))]
    for peer in peers:
        pl.semaphore_signal(barrier, inc=1, device_id=peer, device_id_type=MESH)
    pl.semaphore_wait(barrier, len(peers))
    for c in local:
        c.wait()

    def remote(src, dst, s, t, to):
        return pltpu.make_async_remote_copy(
            src_ref=src, dst_ref=dst, send_sem=s, recv_sem=t, device_id=to, device_id_type=MESH
        )

    sent = []

    def launch(*args):
        c = remote(*args)
        c.start()
        sent.append(c)

    piece = lambda g, c: xg.at[g, pl.ds(c * own, own)]
    for c in range(nc):
        for d in range(1, a):
            ref = wg.at[k, c]
            launch(ref, ref, sw.at[d - 1, c], rw.at[d - 1, c], col_peer(d))
    for d in range(1, b):
        launch(lg.at[m], lg.at[m], sl.at[d - 1], rl.at[d - 1], row_peer(d))

    def pass_on(o, up, go):
        src = piece(o, v)
        to = line(m + 1 if up else m - 1)
        c = remote(src, src, su.at[o, 0 if up else 1], rf.at[o, 0], to)
        pl.when(go)(c.start)

    pass_on(m, True, m < b - 1)
    pass_on(m, False, m > 0)

    def recv_line(t):
        o = jnp.bitwise_xor(m, turn(t))
        src = piece(o, v)
        remote(src, src, sx.at[t, 0], rf.at[o, 0], across(0)).wait_recv()
        pass_on(o, True, (o < m) & (m < b - 1))
        pass_on(o, False, (o > m) & (m > 0))
        for bit in bits:
            remote(src, src, sx.at[t, bit], rf.at[o, bit], (r, flip(v, bit, V))).start()

    def recv_side(t, mask):
        o = jnp.bitwise_xor(m, turn(t))
        low = mask & -mask
        src = piece(o, flip(v, mask, V))
        remote(src, src, sx.at[t, mask], rf.at[o, mask], across(0)).wait_recv()
        for bit in bits:
            if bit < low:
                remote(src, src, sx.at[t, mask | bit], rf.at[o, mask | bit], (r, flip(v, bit, V))).start()

    def recv_chunk(e):
        d, c = e // nc, e % nc
        ref = wg.at[flip(k, d, a), c]
        remote(ref, ref, sw.at[d - 1, c], rw.at[d - 1, c], col_peer(d)).wait_recv()

    def task(which, es):
        for j, (d, h) in enumerate(which):
            p = d * half + h
            g, pr = jnp.bitwise_xor(m, d), jnp.bitwise_xor(v // 2, h)
            xs = xg[g, pl.ds(pr * unit, unit)].reshape(rows, width)
            old = mx[p]
            new = old
            base = []
            for i, e in enumerate(es):
                ke = jnp.bitwise_xor(k, e // nc)
                c = e % nc
                l = jnp.dot(xs, wg[ke, c], preferred_element_type=jnp.float32)
                logit[j, :, i * cw : (i + 1) * cw] = l
                for n in range(0, cw, 128):
                    new = jnp.maximum(new, l[:, n : n + 128])
                low = l.astype(jnp.bfloat16)
                base = (v * G + m * a + ke) * cols + c * cw
                ids = lax.broadcasted_iota(jnp.int32, (cw, slots), 0) + base
                for q in range(unit):
                    hot = (ids == lg[g, pr * unit + q]).astype(jnp.float32).astype(jnp.bfloat16)
                    got = jnp.dot(low[q * frames : (q + 1) * frames], hot, preferred_element_type=jnp.float32)
                    acc[p, q] = acc[p, q] + got
            s = sm[p] * jnp.exp(old - new)
            for n in range(0, len(es) * cw, 128):
                s = s + jnp.exp(logit[j, :, n : n + 128] - new)
            mx[p] = new
            sm[p] = s

    def clear(p, _):
        mx[p] = jnp.full((rows, 128), LOW, jnp.float32)
        sm[p] = jnp.zeros((rows, 128), jnp.float32)
        acc[p] = jnp.zeros((unit, frames, slots), jnp.float32)
        return 0

    def chunks_of(d, h, count):
        lax.fori_loop(0, count // 2, lambda i, _: (task([(d, h)], [2 * i, 2 * i + 1]), 0)[1], 0)
        if count % 2:
            task([(d, h)], [count - 1])

    def pairs_of(count, e):
        at = lambda i: (turn(i // half), i % half)
        lax.fori_loop(0, count // 2, lambda i, _: (task([at(2 * i), at(2 * i + 1)], [e]), 0)[1], 0)
        if count % 2:
            task([at(count - 1)], [e])

    lax.fori_loop(0, pairs, clear, 0)

    events = []
    for t in range(1, b):
        events.append((0.2 * max(t - 1, 1), 0, t, 0))
        events.append((0.2 * t, 1, t, 0))
        for h in range(half):
            events.append((0.2 * t + 0.03 + 0.17 * h, 2, t, h))
    for e in range(nc, chunks - 1):
        events.append(((e - nc + 1) / (chunks - nc), 3, e, 0))
    events.sort()

    lax.fori_loop(0, half, lambda h, _: (chunks_of(0, h, nc), 0)[1], 0)
    have_p, have_e = half, nc
    for _, kind, i, h in events:
        if kind == 0:
            pl.when(inner)(functools.partial(recv_line, i))
        elif kind == 1:
            pl.when(jnp.logical_not(inner))(functools.partial(recv_line, i))
        elif kind == 2:
            if h == 0:
                d = turn(i)
                o = jnp.bitwise_xor(m, d)
                remote(lg.at[o], lg.at[o], sl.at[0], rl.at[d - 1], row_peer(1)).wait_recv()
            if h > 0:
                recv_side(i, 2 * h)
            recv_side(i, 2 * h + 1)
            chunks_of(turn(i), h, have_e)
            have_p += 1
        else:
            recv_chunk(i)
            pairs_of(have_p, i)
            have_e = i + 1

    lane = lax.broadcasted_iota(jnp.int32, (frames, 128), 1)
    tall = 4 * unit

    def merge(p, q):
        odd = lax.broadcasted_iota(jnp.int32, (tall, frames), 0) % 2 == 1
        pt, qt = pltpu.roll(p, 1, 0), pltpu.roll(q, 1, 0)
        top = jnp.maximum(pt, qt)
        total = p * jnp.exp(pt - top) + q * jnp.exp(qt - top)
        return jnp.where(odd, total, jnp.maximum(p, q))

    def finish(n, which):
        tile = jnp.zeros((frames, 128), jnp.float32)
        for j, (d, h) in enumerate(which):
            p = d * half + h
            best = mx[p]
            top = jnp.max(best, 1, keepdims=True)
            total = jnp.sum(sm[p] * jnp.exp(best - top), 1, keepdims=True)
            for q in range(unit):
                part = slice(q * frames, (q + 1) * frames)
                pp[p, q // own, q % own] = acc[p, q].astype(jnp.bfloat16)
                at = 2 * (j * unit + q)
                tile = jnp.where(lane == at, top[part], tile)
                tile = jnp.where(lane == at + 1, total[part], tile)
        st[n] = tile.T[:tall]
        for d, h in which:
            p = d * half + h
            launch(pp.at[p, 1 - side], pin.at[p], sp.at[p], rp.at[p], sibling)
        launch(st.at[n], sin.at[n], ss.at[n], rs.at[n], sibling)

    def join_sibling(n, which):
        for d, h in which:
            p = d * half + h
            remote(pin.at[p], pin.at[p], sp.at[p], rp.at[p], sibling).wait_recv()
            cs[p] = pp[p, side] + pin[p]
            if h:
                launch(cs.at[p], xin.at[d, h - 1], sq.at[p], rq.at[d, h - 1], across(h))
        remote(sin.at[n], sin.at[n], ss.at[n], rs.at[n], sibling).wait_recv()
        cst[n] = merge(st[n], sin[n])
        h = which[0][1]
        if h:
            t = which[0][0] // 2
            launch(cst.at[n], xst.at[t, h - 1], sv.at[n], rv.at[t, h - 1], across(h))

    def join_across(n, which):
        t = which[0][0] // 2
        for d, _ in which:
            total = cs[d * half]
            for h in range(1, half):
                remote(xin.at[d, h - 1], xin.at[d, h - 1], sq.at[0], rq.at[d, h - 1], across(h)).wait_recv()
                total = total + xin[d, h - 1]
            if d:
                xout[d] = total
                launch(xout.at[d], zin.at[d], sz.at[d], rz.at[d], row_peer(d))
            else:
                zin[d] = total
        tile = cst[n]
        for h in range(1, half):
            remote(xst.at[t, h - 1], xst.at[t, h - 1], sv.at[0], rv.at[t, h - 1], across(h)).wait_recv()
            tile = merge(tile, xst[t, h - 1])
        zsrc[t] = tile
        for d, _ in which:
            if d:
                launch(zsrc.at[t], zst.at[d], sy.at[d], ry.at[d], row_peer(d))
            else:
                zst[d] = tile

    recv_chunk(chunks - 1)
    blocks = [[(2 * t + 1, h), (2 * t, h)] for h in reversed(range(half)) for t in reversed(range(b // 2))]
    for n, which in enumerate(blocks):
        task(which, [chunks - 1])
        finish(n, which)
        if n:
            join_sibling(n - 1, blocks[n - 1])
    last = len(blocks) - 1
    join_sibling(last, blocks[last])
    for n, which in enumerate(blocks):
        if which[0][1] == 0:
            join_across(n, which)

    for q in range(own):
        got = zin[0, q]
        for d in range(1, b):
            if q == 0:
                remote(zin.at[d], zin.at[d], sz.at[d], rz.at[d], row_peer(d)).wait_recv()
                remote(zst.at[d], zst.at[d], sy.at[d], ry.at[d], row_peer(d)).wait_recv()
            got = got + zin[d, q]
        pick_ref[q] = got
        tops, sums = [], []
        for d in range(b):
            at = 2 * ((1 - d % 2) * unit + side * own + q)
            tops.append(zst[d, pl.ds(at, 1), :])
            sums.append(zst[d, pl.ds(at + 1, 1), :])
        top = tops[0]
        for one in tops[1:]:
            top = jnp.maximum(top, one)
        total = jnp.zeros_like(top)
        for one, part in zip(tops, sums):
            total = total + part * jnp.exp(one - top)
        stat_ref[q] = jnp.broadcast_to(top + jnp.log(total), (8, frames))

    for c in sent:
        c.wait_send()
    for t in range(1, b):
        o = jnp.bitwise_xor(m, turn(t))
        for mask in range(1, V):
            src = piece(o, v)
            remote(src, src, sx.at[t, mask], rf.at[o, mask], across(0)).wait_send()
    for o in range(b):
        src = piece(o, v)
        pl.when((o <= m) & (m < b - 1))(remote(src, src, su.at[o, 0], rf.at[o, 0], across(0)).wait_send)
        pl.when((o >= m) & (m > 0))(remote(src, src, su.at[o, 1], rf.at[o, 0], across(0)).wait_send)


def align_kernel(alen, tlen, pick, stat, lp_ref, out_ref):
    own, frames, slots = pick.shape
    lane = lax.broadcasted_iota(jnp.int32, (1, slots), 1)
    for q in range(own):
        norm = jnp.broadcast_to(stat[q, 0:1, :], (slots, frames)).T
        lp_ref[q] = pick[q].astype(jnp.float32) - norm
        last = alen[q] - 1
        first = jnp.where(lane == 0, lp_ref[q, 0:1, :], NEG)

        def block(t, steps, cur, best):
            emit = [lp_ref[q, pl.ds(t + i, 1), :] for i in range(steps)]
            rolled = [[e if c == 0 else pltpu.roll(e, c, 1) for c in range(steps - i)] for i, e in enumerate(emit)]
            moved = [cur] + [jnp.where(lane < c, NEG, pltpu.roll(cur, c, 1)) for c in range(1, steps + 1)]
            for i in range(steps):
                moved = [jnp.maximum(moved[c], moved[c + 1]) + rolled[i][c] for c in range(steps - i)]
                best = jnp.where(last == t + i, moved[0], best)
            return moved[0], best

        whole = (frames - 1) // run
        cur, best = lax.fori_loop(0, whole, lambda i, c: block(1 + i * run, run, *c), (first, first))
        if (frames - 1) % run:
            best = block(1 + whole * run, (frames - 1) % run, cur, best)[1]
        score = jnp.sum(jnp.where(lane == tlen[q] - 1, best, 0.0), 1, keepdims=True)
        out_ref[q] = jnp.broadcast_to(score, (8, 128))


def body(features, head_weight, labels, audio_len, transcript_len):
    rec_dev, frames, width = features.shape
    cols = head_weight.shape[1]
    slots = labels.shape[1]
    G, V = lax.axis_size("rec"), lax.axis_size("vocab")
    best = None
    a = 2
    while a < G:
        cost = (a - 1) * width * cols + (G // a - 1) * features.size
        if G % a == 0 and (best is None or cost < best[0]):
            best = (cost, a)
        a *= 2
    a = best[1]
    b = G // a
    own = rec_dev // V
    vmem = pl.BlockSpec(memory_space=pltpu.VMEM)
    hbm = pl.BlockSpec(memory_space=pl.ANY)
    smem = pl.BlockSpec(memory_space=pltpu.SMEM)
    dma = pltpu.SemaphoreType.DMA
    cw = min(256, cols)
    nc = cols // cw
    unit = 2 * own
    pairs = b * (V // 2)
    rows = unit * frames
    bf, f32 = jnp.bfloat16, jnp.float32
    half = V // 2
    tall = 4 * unit
    one = (own, frames, slots)
    pick, stat = pl.pallas_call(
        functools.partial(emit_kernel, a, b, V),
        out_shape=(jax.ShapeDtypeStruct(one, bf), jax.ShapeDtypeStruct((own, 8, frames), f32)),
        in_specs=[hbm] * 3,
        out_specs=(vmem, vmem),
        scratch_shapes=[
            pltpu.VMEM((b,) + features.shape, features.dtype),
            pltpu.VMEM((a, nc, width, cw), head_weight.dtype),
            pltpu.VMEM((b, rec_dev, 1, slots), jnp.int32),
            pltpu.VMEM((pairs, rows, 128), f32),
            pltpu.VMEM((pairs, rows, 128), f32),
            pltpu.VMEM((pairs, unit, frames, slots), f32),
            pltpu.VMEM((2, rows, 2 * cw), f32),
            pltpu.VMEM((pairs, 2) + one, bf),
            pltpu.VMEM((pairs,) + one, bf),
            pltpu.VMEM((pairs,) + one, bf),
            pltpu.VMEM((b, half - 1) + one, bf),
            pltpu.VMEM((b,) + one, bf),
            pltpu.VMEM((b,) + one, bf),
            pltpu.VMEM((pairs // 2, tall, frames), f32),
            pltpu.VMEM((pairs // 2, tall, frames), f32),
            pltpu.VMEM((pairs // 2, tall, frames), f32),
            pltpu.VMEM((b // 2, half - 1, tall, frames), f32),
            pltpu.VMEM((b // 2, tall, frames), f32),
            pltpu.VMEM((b, tall, frames), f32),
            dma((a - 1, nc)), dma((a - 1, nc)), dma((b - 1,)), dma((b - 1,)),
            dma((b, 2)), dma((b, V)), dma((b, V)),
            dma((pairs,)), dma((pairs,)), dma((pairs // 2,)), dma((pairs // 2,)),
            dma((pairs,)), dma((b, half - 1)), dma((pairs // 2,)), dma((b // 2, half - 1)),
            dma((b,)), dma((b,)), dma((b,)), dma((b,)), dma((2 + nc,)),
        ],
        compiler_params=pltpu.CompilerParams(
            collective_id=0, has_side_effects=True, vmem_limit_bytes=60 * 1024 * 1024
        ),
        name="emit",
    )(features, head_weight, labels.reshape(rec_dev, 1, slots))

    log_prob, score = pl.pallas_call(
        align_kernel,
        out_shape=(
            jax.ShapeDtypeStruct((own, frames, slots), jnp.float32),
            jax.ShapeDtypeStruct((own, 8, 128), jnp.float32),
        ),
        in_specs=[smem, smem, vmem, vmem],
        out_specs=(vmem, vmem),
        name="align",
    )(audio_len, transcript_len, pick, stat)
    return log_prob, score[:, 0, 0]


def solution(mesh):
    return jax.shard_map(
        body,
        mesh=mesh,
        in_specs=(
            P("rec", None, None),
            P(None, ("vocab", "rec")),
            P("rec", None),
            P(("rec", "vocab")),
            P(("rec", "vocab")),
        ),
        out_specs=(P(("rec", "vocab"), None, None), P(("rec", "vocab"))),
        check_vma=False,
    )
```

```python
import functools
import jax
import jax.numpy as jnp
from jax import lax
from jax.experimental import pallas as pl
from jax.experimental.pallas import tpu as pltpu
from jax.sharding import PartitionSpec as P

MESH = pl.DeviceIdType.MESH
NEG = -1e30
LOW = -3e38
run = 8


def bits_of(size):
    bits = []
    bit = size // 2
    while bit >= 1:
        bits.append(bit)
        bit //= 2
    return bits


def flip(v, mask, size):
    for bit in bits_of(size):
        if mask & bit:
            v = v + bit * (1 - 2 * ((v // bit) % 2))
    return v


def best_path(q, last, goal, lp_ref, right, left):
    own, frames, slots = lp_ref.shape
    lane = lax.broadcasted_iota(jnp.int32, (1, slots), 1)
    whole = lp_ref[q]
    for c in range(1, run):
        right[c - 1] = pltpu.roll(whole, c, 1)
    for c in range(1, run + 1):
        left[c - 1] = pltpu.roll(whole, slots - c, 1)
    mid = frames // 2

    def row(shifted, c, t):
        return lp_ref[q, pl.ds(t, 1), :] if c == 0 else shifted[c - 1, pl.ds(t, 1), :]

    def forward(t, steps, cur, best):
        moved = [cur] + [jnp.where(lane < c, NEG, pltpu.roll(cur, c, 1)) for c in range(1, steps + 1)]
        for i in range(steps):
            moved = [jnp.maximum(moved[c], moved[c + 1]) + row(right, c, t + i) for c in range(steps - i)]
            best = jnp.where(last == t + i, moved[0], best)
        return moved[0], best

    ends = [jnp.where(lane + c == goal, 0.0, NEG) for c in range(run + 1)]

    def backward(t, steps, cur):
        moved = [cur] + [jnp.where(lane >= slots - c, NEG, pltpu.roll(cur, slots - c, 1)) for c in range(1, steps + 1)]
        for i in range(steps):
            moved = [jnp.where(last == t - i, ends[c], moved[c]) + row(left, c, t - i) for c in range(steps - i + 1)]
            moved = [jnp.maximum(moved[c], moved[c + 1]) for c in range(steps - i)]
        return moved[0]

    first = jnp.where(lane == 0, lp_ref[q, 0:1, :], NEG)
    ahead, behind = mid - 1, frames - mid
    count = min(ahead, behind) // run

    def both(i, carry):
        cur, best, tail = carry
        cur, best = forward(1 + i * run, run, cur, best)
        return cur, best, backward(frames - 1 - i * run, run, tail)

    cur, best, tail = lax.fori_loop(0, count, both, (first, first, jnp.full((1, slots), NEG, jnp.float32)))
    done = count * run
    at = done
    while at < ahead:
        cur, best = forward(1 + at, min(run, ahead - at), cur, best)
        at += min(run, ahead - at)
    at = done
    while at < behind:
        tail = backward(frames - 1 - at, min(run, behind - at), tail)
        at += min(run, behind - at)
    early = jnp.sum(jnp.where(lane == goal, best, 0.0), 1, keepdims=True)
    late = jnp.max(cur + tail, 1, keepdims=True)
    return jnp.where(last < mid, early, late)


def emit_kernel(
    a, b, V, x, w, lab, pick_ref, stat_ref, xg, wg, lg, mx, sm, acc, logit,
    pp, pin, cs, xin, xout, zin, st, sin, cst, xst, zsrc, zst,
    sw, rw, sl, rl, su, sx, rf, sp, rp, ss, rs, sq, rq, sv, rv, sz, rz, sy, ry, loc,
):
    r = lax.axis_index("rec")
    v = lax.axis_index("vocab")
    G = a * b
    m, k = r // a, r % a
    rec_dev, frames, width = x.shape
    own = rec_dev // V
    nc, cw = wg.shape[1], wg.shape[3]
    cols = nc * cw
    slots = lab.shape[2]
    half = V // 2
    side = v % 2
    bits = bits_of(V)
    unit = 2 * own
    rows = unit * frames
    pairs = b * half
    chunks = a * nc

    def among(values, i):
        out = values[0]
        for j in range(1, len(values)):
            out = jnp.where(i == j, values[j], out)
        return out

    near = [sorted(range(b), key=lambda o: (abs(o - i), o)) for i in range(b)]
    turns = [among([near[i][t] ^ i for i in range(b)], m) for t in range(b)]
    turn = lambda t: turns[t] if isinstance(t, int) else among(turns, t)
    inner = (m > 0) & (m < b - 1)

    col_peer = lambda d: (m * a + flip(k, d, a), v)
    row_peer = lambda d: (flip(m, d, b) * a + k, v)
    line = lambda at: (at * a + k, v)
    sibling = (r, flip(v, 1, V))
    across = lambda h: (r, flip(v, 2 * h, V))

    local = [pltpu.make_async_copy(x, xg.at[m], loc.at[0]), pltpu.make_async_copy(lab, lg.at[m], loc.at[1])]
    for c in range(nc):
        local.append(pltpu.make_async_copy(w.at[:, pl.ds(c * cw, cw)], wg.at[k, c], loc.at[2 + c]))
    for c in local:
        c.start()

    barrier = pltpu.get_barrier_semaphore()
    peers = [col_peer(d) for d in range(1, a)]
    peers += [(r, flip(v, mask, V)) for mask in sorted(set(bits + [2 * h for h in range(1, half)]))]

    def greet(peer):
        pl.semaphore_signal(barrier, inc=1, device_id=peer, device_id_type=MESH)

    for peer in peers:
        greet(peer)
    pl.when(m < b - 1)(lambda: greet(line(m + 1)))
    pl.when(m > 0)(lambda: greet(line(m - 1)))
    pl.semaphore_wait(barrier, len(peers) + jnp.minimum(m, 1) + jnp.minimum(b - 1 - m, 1))
    local[0].wait()
    local[1].wait()

    def remote(src, dst, s, t, to):
        return pltpu.make_async_remote_copy(
            src_ref=src, dst_ref=dst, send_sem=s, recv_sem=t, device_id=to, device_id_type=MESH
        )

    sent = []

    def launch(*args):
        c = remote(*args)
        c.start()
        sent.append(c)

    piece = lambda g, c: xg.at[g, pl.ds(c * own, own)]
    for c in range(nc):
        for d in range(1, a):
            ref = wg.at[k, c]
            launch(w.at[:, pl.ds(c * cw, cw)], ref, sw.at[d - 1, c], rw.at[d - 1, c], col_peer(d))
    def pass_on(o, up, go):
        src = piece(o, v)
        to = line(m + 1 if up else m - 1)
        c = remote(src, src, su.at[o, 0 if up else 1], rf.at[o, 0], to)
        tags = remote(lg.at[o], lg.at[o], sl.at[o, 0 if up else 1], rl.at[o], to)

        def start():
            tags.start()
            c.start()

        pl.when(go)(start)

    pass_on(m, True, m < b - 1)
    pass_on(m, False, m > 0)

    def recv_line(t):
        o = jnp.bitwise_xor(m, turn(t))
        src = piece(o, v)
        remote(lg.at[o], lg.at[o], sl.at[o, 0], rl.at[o], across(0)).wait_recv()
        remote(src, src, sx.at[t, 0], rf.at[o, 0], across(0)).wait_recv()
        pass_on(o, True, (o < m) & (m < b - 1))
        pass_on(o, False, (o > m) & (m > 0))
        for bit in bits:
            remote(src, src, sx.at[t, bit], rf.at[o, bit], (r, flip(v, bit, V))).start()

    def recv_side(t, mask):
        o = jnp.bitwise_xor(m, turn(t))
        low = mask & -mask
        src = piece(o, flip(v, mask, V))
        remote(src, src, sx.at[t, mask], rf.at[o, mask], across(0)).wait_recv()
        for bit in bits:
            if bit < low:
                remote(src, src, sx.at[t, mask | bit], rf.at[o, mask | bit], (r, flip(v, bit, V))).start()

    def recv_chunk(e):
        d, c = e // nc, e % nc
        ref = wg.at[flip(k, d, a), c]
        remote(ref, ref, sw.at[d - 1, c], rw.at[d - 1, c], col_peer(d)).wait_recv()

    def task(which, es):
        for j, (d, h) in enumerate(which):
            p = d * half + h
            g, pr = jnp.bitwise_xor(m, d), jnp.bitwise_xor(v // 2, h)
            xs = xg[g, pl.ds(pr * unit, unit)].reshape(rows, width)
            old = mx[p]
            new = old
            base = []
            for i, e in enumerate(es):
                ke = jnp.bitwise_xor(k, e // nc)
                c = e % nc
                l = jnp.dot(xs, wg[ke, c], preferred_element_type=jnp.float32)
                logit[j, :, i * cw : (i + 1) * cw] = l
                for n in range(0, cw, 128):
                    new = jnp.maximum(new, l[:, n : n + 128])
                low = l.astype(jnp.bfloat16)
                base = (v * G + m * a + ke) * cols + c * cw
                ids = lax.broadcasted_iota(jnp.int32, (cw, slots), 0) + base
                for q in range(unit):
                    hot = (ids == lg[g, pr * unit + q]).astype(jnp.float32).astype(jnp.bfloat16)
                    got = jnp.dot(low[q * frames : (q + 1) * frames], hot, preferred_element_type=jnp.float32)
                    acc[p, q] = acc[p, q] + got
            s = sm[p] * jnp.exp(old - new)
            for n in range(0, len(es) * cw, 128):
                s = s + jnp.exp(logit[j, :, n : n + 128] - new)
            mx[p] = new
            sm[p] = s

    def clear(p, _):
        mx[p] = jnp.full((rows, 128), LOW, jnp.float32)
        sm[p] = jnp.zeros((rows, 128), jnp.float32)
        acc[p] = jnp.zeros((unit, frames, slots), jnp.float32)
        return 0

    def chunks_of(d, h, count):
        lax.fori_loop(0, count // 2, lambda i, _: (task([(d, h)], [2 * i, 2 * i + 1]), 0)[1], 0)
        if count % 2:
            task([(d, h)], [count - 1])

    def pairs_of(count, e):
        at = lambda i: (turn(i // half), i % half)
        lax.fori_loop(0, count // 2, lambda i, _: (task([at(2 * i), at(2 * i + 1)], [e]), 0)[1], 0)
        if count % 2:
            task([at(count - 1)], [e])

    for c in local[2:]:
        c.wait()
    lax.fori_loop(0, pairs, clear, 0)

    events = []
    for t in range(1, b):
        events.append((0.2 * max(t - 1, 1), 0, t, 0))
        events.append((0.2 * t, 1, t, 0))
        for h in range(half):
            events.append((0.2 * t + 0.03 + 0.17 * h, 2, t, h))
    for e in range(nc, chunks - 1):
        events.append(((e - nc + 1) / (chunks - nc), 3, e, 0))
    events.sort()

    lax.fori_loop(0, half, lambda h, _: (chunks_of(0, h, nc), 0)[1], 0)
    have_p, have_e = half, nc
    for _, kind, i, h in events:
        if kind == 0:
            pl.when(inner)(functools.partial(recv_line, i))
        elif kind == 1:
            pl.when(jnp.logical_not(inner))(functools.partial(recv_line, i))
        elif kind == 2:
            if h > 0:
                recv_side(i, 2 * h)
            recv_side(i, 2 * h + 1)
            chunks_of(turn(i), h, have_e)
            have_p += 1
        else:
            recv_chunk(i)
            pairs_of(have_p, i)
            have_e = i + 1

    lane = lax.broadcasted_iota(jnp.int32, (frames, 128), 1)
    tall = 4 * unit

    def merge(p, q):
        odd = lax.broadcasted_iota(jnp.int32, (tall, frames), 0) % 2 == 1
        pt, qt = pltpu.roll(p, 1, 0), pltpu.roll(q, 1, 0)
        top = jnp.maximum(pt, qt)
        total = p * jnp.exp(pt - top) + q * jnp.exp(qt - top)
        return jnp.where(odd, total, jnp.maximum(p, q))

    def finish(n, which):
        tile = jnp.zeros((frames, 128), jnp.float32)
        for j, (d, h) in enumerate(which):
            p = d * half + h
            best = mx[p]
            top = jnp.max(best, 1, keepdims=True)
            total = jnp.sum(sm[p] * jnp.exp(best - top), 1, keepdims=True)
            for q in range(unit):
                part = slice(q * frames, (q + 1) * frames)
                pp[p, q // own, q % own] = acc[p, q].astype(jnp.bfloat16)
                at = 2 * (j * unit + q)
                tile = jnp.where(lane == at, top[part], tile)
                tile = jnp.where(lane == at + 1, total[part], tile)
        st[n] = tile.T[:tall]
        for d, h in which:
            p = d * half + h
            launch(pp.at[p, 1 - side], pin.at[p], sp.at[p], rp.at[p], sibling)
        launch(st.at[n], sin.at[n], ss.at[n], rs.at[n], sibling)

    def join_sibling(n, which):
        for d, h in which:
            p = d * half + h
            remote(pin.at[p], pin.at[p], sp.at[p], rp.at[p], sibling).wait_recv()
            cs[p] = pp[p, side] + pin[p]
            if h:
                launch(cs.at[p], xin.at[d, h - 1], sq.at[p], rq.at[d, h - 1], across(h))
        remote(sin.at[n], sin.at[n], ss.at[n], rs.at[n], sibling).wait_recv()
        cst[n] = merge(st[n], sin[n])
        h = which[0][1]
        if h:
            t = which[0][0] // 2
            launch(cst.at[n], xst.at[t, h - 1], sv.at[n], rv.at[t, h - 1], across(h))

    def join_across(n, which):
        t = which[0][0] // 2
        for d, _ in which:
            total = cs[d * half]
            for h in range(1, half):
                remote(xin.at[d, h - 1], xin.at[d, h - 1], sq.at[0], rq.at[d, h - 1], across(h)).wait_recv()
                total = total + xin[d, h - 1]
            if d:
                xout[d] = total
                launch(xout.at[d], zin.at[d], sz.at[d], rz.at[d], row_peer(d))
            else:
                zin[d] = total
        tile = cst[n]
        for h in range(1, half):
            remote(xst.at[t, h - 1], xst.at[t, h - 1], sv.at[0], rv.at[t, h - 1], across(h)).wait_recv()
            tile = merge(tile, xst[t, h - 1])
        zsrc[t] = tile
        for d, _ in which:
            if d:
                launch(zsrc.at[t], zst.at[d], sy.at[d], ry.at[d], row_peer(d))
            else:
                zst[d] = tile

    for c in sent[: (a - 1) * (nc - 1)]:
        c.wait_send()
    del sent[: (a - 1) * (nc - 1)]
    for t in range(1, b):
        o = jnp.bitwise_xor(m, turn(t))
        for mask in range(1, V):
            src = piece(o, v)
            remote(src, src, sx.at[t, mask], rf.at[o, mask], across(0)).wait_send()
    for o in range(b):
        src, tag = piece(o, v), lg.at[o]
        for i, go in enumerate(((o <= m) & (m < b - 1), (o >= m) & (m > 0))):
            pl.when(go)(remote(src, src, su.at[o, i], rf.at[o, 0], across(0)).wait_send)
            pl.when(go)(remote(tag, tag, sl.at[o, i], rl.at[o], across(0)).wait_send)
    recv_chunk(chunks - 1)
    blocks = [[(2 * t + 1, h), (2 * t, h)] for h in reversed(range(half)) for t in reversed(range(b // 2))]
    for n, which in enumerate(blocks):
        task(which, [chunks - 1])
        finish(n, which)
        if n:
            join_sibling(n - 1, blocks[n - 1])
    last = len(blocks) - 1
    join_sibling(last, blocks[last])
    for n, which in enumerate(blocks):
        if which[0][1] == 0:
            join_across(n, which)

    for q in range(own):
        got = zin[0, q]
        for d in range(1, b):
            if q == 0:
                remote(zin.at[d], zin.at[d], sz.at[d], rz.at[d], row_peer(d)).wait_recv()
                remote(zst.at[d], zst.at[d], sy.at[d], ry.at[d], row_peer(d)).wait_recv()
            got = got + zin[d, q]
        tops, sums = [], []
        for d in range(b):
            at = 2 * ((1 - d % 2) * unit + side * own + q)
            tops.append(zst[d, pl.ds(at, 1), :])
            sums.append(zst[d, pl.ds(at + 1, 1), :])
        top = tops[0]
        for one in tops[1:]:
            top = jnp.maximum(top, one)
        total = jnp.zeros_like(top)
        for one, part in zip(tops, sums):
            total = total + part * jnp.exp(one - top)
        pick_ref[q] = got
        stat_ref[q] = jnp.broadcast_to(top + jnp.log(total), (8, frames))

    for c in sent:
        c.wait_send()


def align_kernel(alen, tlen, pick, stat, lp_ref, out_ref, right, left):
    own, frames, slots = pick.shape
    lane = lax.broadcasted_iota(jnp.int32, (1, own), 1)
    scores = jnp.zeros((1, own), jnp.float32)
    for q in range(own):
        norm = jnp.broadcast_to(stat[q, 0:1, :], (slots, frames)).T
        lp_ref[q] = pick[q].astype(jnp.float32) - norm
        last, goal = alen[0:1, q : q + 1] - 1, tlen[0:1, q : q + 1] - 1
        scores = jnp.where(lane == q, best_path(q, last, goal, lp_ref, right, left), scores)
    out_ref[...] = scores


def body(features, head_weight, labels, audio_len, transcript_len):
    rec_dev, frames, width = features.shape
    cols = head_weight.shape[1]
    slots = labels.shape[1]
    G, V = lax.axis_size("rec"), lax.axis_size("vocab")
    best = None
    a = 2
    while a < G:
        cost = (a - 1) * width * cols + (G // a - 1) * features.size
        if G % a == 0 and (best is None or cost < best[0]):
            best = (cost, a)
        a *= 2
    a = best[1]
    b = G // a
    own = rec_dev // V
    vmem = pl.BlockSpec(memory_space=pltpu.VMEM)
    hbm = pl.BlockSpec(memory_space=pl.ANY)
    dma = pltpu.SemaphoreType.DMA
    cw = min(256, cols)
    nc = cols // cw
    unit = 2 * own
    pairs = b * (V // 2)
    rows = unit * frames
    bf, f32 = jnp.bfloat16, jnp.float32
    half = V // 2
    tall = 4 * unit
    one = (own, frames, slots)
    pick, stat = pl.pallas_call(
        functools.partial(emit_kernel, a, b, V),
        out_shape=(jax.ShapeDtypeStruct(one, bf), jax.ShapeDtypeStruct((own, 8, frames), f32)),
        in_specs=[hbm] * 3,
        out_specs=(vmem, vmem),
        scratch_shapes=[
            pltpu.VMEM((b,) + features.shape, features.dtype),
            pltpu.VMEM((a, nc, width, cw), head_weight.dtype),
            pltpu.VMEM((b, rec_dev, 1, slots), jnp.int32),
            pltpu.VMEM((pairs, rows, 128), f32),
            pltpu.VMEM((pairs, rows, 128), f32),
            pltpu.VMEM((pairs, unit, frames, slots), f32),
            pltpu.VMEM((2, rows, 2 * cw), f32),
            pltpu.VMEM((pairs, 2) + one, bf),
            pltpu.VMEM((pairs,) + one, bf),
            pltpu.VMEM((pairs,) + one, bf),
            pltpu.VMEM((b, half - 1) + one, bf),
            pltpu.VMEM((b,) + one, bf),
            pltpu.VMEM((b,) + one, bf),
            pltpu.VMEM((pairs // 2, tall, frames), f32),
            pltpu.VMEM((pairs // 2, tall, frames), f32),
            pltpu.VMEM((pairs // 2, tall, frames), f32),
            pltpu.VMEM((b // 2, half - 1, tall, frames), f32),
            pltpu.VMEM((b // 2, tall, frames), f32),
            pltpu.VMEM((b, tall, frames), f32),
            dma((a - 1, nc)), dma((a - 1, nc)), dma((b, 2)), dma((b,)),
            dma((b, 2)), dma((b, V)), dma((b, V)),
            dma((pairs,)), dma((pairs,)), dma((pairs // 2,)), dma((pairs // 2,)),
            dma((pairs,)), dma((b, half - 1)), dma((pairs // 2,)), dma((b // 2, half - 1)),
            dma((b,)), dma((b,)), dma((b,)), dma((b,)), dma((2 + nc,)),
        ],
        compiler_params=pltpu.CompilerParams(
            collective_id=0, has_side_effects=True, vmem_limit_bytes=60 * 1024 * 1024
        ),
        name="emit",
    )(features, head_weight, labels.reshape(rec_dev, 1, slots))

    log_prob, score = pl.pallas_call(
        align_kernel,
        out_shape=(jax.ShapeDtypeStruct(one, f32), jax.ShapeDtypeStruct((1, own), f32)),
        in_specs=[vmem] * 4,
        out_specs=(vmem, vmem),
        scratch_shapes=[pltpu.VMEM((run - 1, frames, slots), f32), pltpu.VMEM((run, frames, slots), f32)],
        name="align",
    )(audio_len.reshape(1, own), transcript_len.reshape(1, own), pick, stat)
    return log_prob, score.reshape(own)


def solution(mesh):
    return jax.shard_map(
        body,
        mesh=mesh,
        in_specs=(
            P("rec", None, None),
            P(None, ("vocab", "rec")),
            P("rec", None),
            P(("rec", "vocab")),
            P(("rec", "vocab")),
        ),
        out_specs=(P(("rec", "vocab"), None, None), P(("rec", "vocab"))),
        check_vma=False,
    )
```

```python
import functools
import jax
import jax.numpy as jnp
from jax import lax
from jax.experimental import pallas as pl
from jax.experimental.pallas import tpu as pltpu
from jax.sharding import PartitionSpec as P

MESH = pl.DeviceIdType.MESH
NEG = -1e30
LOW = -3e38
run = 8


def bits_of(size):
    bits = []
    bit = size // 2
    while bit >= 1:
        bits.append(bit)
        bit //= 2
    return bits


def flip(v, mask, size):
    for bit in bits_of(size):
        if mask & bit:
            v = v + bit * (1 - 2 * ((v // bit) % 2))
    return v


def best_path(q, last, goal, lp_ref, right, left):
    own, frames, slots = lp_ref.shape
    lane = lax.broadcasted_iota(jnp.int32, (1, slots), 1)
    whole = lp_ref[q]
    for c in range(1, run):
        right[c - 1] = pltpu.roll(whole, c, 1)
    for c in range(1, run + 1):
        left[c - 1] = pltpu.roll(whole, slots - c, 1)
    mid = frames // 2

    def row(shifted, c, t):
        return lp_ref[q, pl.ds(t, 1), :] if c == 0 else shifted[c - 1, pl.ds(t, 1), :]

    def forward(t, steps, cur, best):
        moved = [cur] + [jnp.where(lane < c, NEG, pltpu.roll(cur, c, 1)) for c in range(1, steps + 1)]
        for i in range(steps):
            moved = [jnp.maximum(moved[c], moved[c + 1]) + row(right, c, t + i) for c in range(steps - i)]
            best = jnp.where(last == t + i, moved[0], best)
        return moved[0], best

    ends = [jnp.where(lane + c == goal, 0.0, NEG) for c in range(run + 1)]

    def backward(t, steps, cur):
        moved = [cur] + [jnp.where(lane >= slots - c, NEG, pltpu.roll(cur, slots - c, 1)) for c in range(1, steps + 1)]
        for i in range(steps):
            moved = [jnp.where(last == t - i, ends[c], moved[c]) + row(left, c, t - i) for c in range(steps - i + 1)]
            moved = [jnp.maximum(moved[c], moved[c + 1]) for c in range(steps - i)]
        return moved[0]

    first = jnp.where(lane == 0, lp_ref[q, 0:1, :], NEG)
    ahead, behind = mid - 1, frames - mid
    count = min(ahead, behind) // run

    def both(i, carry):
        cur, best, tail = carry
        cur, best = forward(1 + i * run, run, cur, best)
        return cur, best, backward(frames - 1 - i * run, run, tail)

    cur, best, tail = lax.fori_loop(0, count, both, (first, first, jnp.full((1, slots), NEG, jnp.float32)))
    done = count * run
    at = done
    while at < ahead:
        cur, best = forward(1 + at, min(run, ahead - at), cur, best)
        at += min(run, ahead - at)
    at = done
    while at < behind:
        tail = backward(frames - 1 - at, min(run, behind - at), tail)
        at += min(run, behind - at)
    early = jnp.sum(jnp.where(lane == goal, best, 0.0), 1, keepdims=True)
    late = jnp.max(cur + tail, 1, keepdims=True)
    return jnp.where(last < mid, early, late)


def emit_kernel(
    a, b, V, x, w, lab, pick_ref, stat_ref, xg, wg, lg, mx, sm, acc, logit,
    pp, pin, cs, xin, xout, zin, st, sin, cst, xst, zsrc, zst,
    sw, rw, sl, rl, su, sx, rf, sp, rp, ss, rs, sq, rq, sv, rv, sz, rz, sy, ry, loc,
):
    r = lax.axis_index("rec")
    v = lax.axis_index("vocab")
    G = a * b
    m, k = r // a, r % a
    rec_dev, frames, width = x.shape
    own = rec_dev // V
    nc, cw = wg.shape[1], wg.shape[3]
    cols = nc * cw
    slots = lab.shape[2]
    half = V // 2
    side = v % 2
    bits = bits_of(V)
    unit = 2 * own
    rows = unit * frames
    pairs = b * half
    chunks = a * nc

    def among(values, i):
        out = values[0]
        for j in range(1, len(values)):
            out = jnp.where(i == j, values[j], out)
        return out

    near = [sorted(range(b), key=lambda o: (abs(o - i), o)) for i in range(b)]
    turns = [among([near[i][t] ^ i for i in range(b)], m) for t in range(b)]
    turn = lambda t: turns[t] if isinstance(t, int) else among(turns, t)
    inner = (m > 0) & (m < b - 1)

    col_peer = lambda d: (m * a + flip(k, d, a), v)
    row_peer = lambda d: (flip(m, d, b) * a + k, v)
    line = lambda at: (at * a + k, v)
    sibling = (r, flip(v, 1, V))
    across = lambda h: (r, flip(v, 2 * h, V))

    local = [pltpu.make_async_copy(x, xg.at[m], loc.at[0]), pltpu.make_async_copy(lab, lg.at[m], loc.at[1])]
    for c in range(nc):
        local.append(pltpu.make_async_copy(w.at[:, pl.ds(c * cw, cw)], wg.at[k, c], loc.at[2 + c]))
    for c in local:
        c.start()

    barrier = pltpu.get_barrier_semaphore()
    peers = [col_peer(d) for d in range(1, a)]
    peers += [(r, flip(v, mask, V)) for mask in sorted(set(bits + [2 * h for h in range(1, half)]))]

    def greet(peer):
        pl.semaphore_signal(barrier, inc=1, device_id=peer, device_id_type=MESH)

    for peer in peers:
        greet(peer)
    pl.when(m < b - 1)(lambda: greet(line(m + 1)))
    pl.when(m > 0)(lambda: greet(line(m - 1)))
    pl.semaphore_wait(barrier, len(peers) + jnp.minimum(m, 1) + jnp.minimum(b - 1 - m, 1))

    def remote(src, dst, s, t, to):
        return pltpu.make_async_remote_copy(
            src_ref=src, dst_ref=dst, send_sem=s, recv_sem=t, device_id=to, device_id_type=MESH
        )

    sent = []

    def launch(*args):
        c = remote(*args)
        c.start()
        sent.append(c)

    piece = lambda g, c: xg.at[g, pl.ds(c * own, own)]
    for c in range(nc):
        for d in range(1, a):
            ref = wg.at[k, c]
            launch(w.at[:, pl.ds(c * cw, cw)], ref, sw.at[d - 1, c], rw.at[d - 1, c], col_peer(d))
    def pass_on(o, up, go):
        src = piece(o, v)
        to = line(m + 1 if up else m - 1)
        c = remote(src, src, su.at[o, 0 if up else 1], rf.at[o, 0], to)
        tags = remote(lg.at[o], lg.at[o], sl.at[o, 0 if up else 1], rl.at[o], to)

        def start():
            tags.start()
            c.start()

        pl.when(go)(start)

    local[0].wait()
    local[1].wait()
    pass_on(m, True, m < b - 1)
    pass_on(m, False, m > 0)

    def recv_line(t):
        o = jnp.bitwise_xor(m, turn(t))
        src = piece(o, v)
        remote(lg.at[o], lg.at[o], sl.at[o, 0], rl.at[o], across(0)).wait_recv()
        remote(src, src, sx.at[t, 0], rf.at[o, 0], across(0)).wait_recv()
        pass_on(o, True, (o < m) & (m < b - 1))
        pass_on(o, False, (o > m) & (m > 0))
        for bit in bits:
            remote(src, src, sx.at[t, bit], rf.at[o, bit], (r, flip(v, bit, V))).start()

    def recv_side(t, mask):
        o = jnp.bitwise_xor(m, turn(t))
        low = mask & -mask
        src = piece(o, flip(v, mask, V))
        remote(src, src, sx.at[t, mask], rf.at[o, mask], across(0)).wait_recv()
        for bit in bits:
            if bit < low:
                remote(src, src, sx.at[t, mask | bit], rf.at[o, mask | bit], (r, flip(v, bit, V))).start()

    def recv_chunk(e):
        d, c = e // nc, e % nc
        ref = wg.at[flip(k, d, a), c]
        remote(ref, ref, sw.at[d - 1, c], rw.at[d - 1, c], col_peer(d)).wait_recv()

    def task(which, es):
        for j, (d, h) in enumerate(which):
            p = d * half + h
            g, pr = jnp.bitwise_xor(m, d), jnp.bitwise_xor(v // 2, h)
            xs = xg[g, pl.ds(pr * unit, unit)].reshape(rows, width)
            old = mx[p]
            new = old
            base = []
            for i, e in enumerate(es):
                ke = jnp.bitwise_xor(k, e // nc)
                c = e % nc
                l = jnp.dot(xs, wg[ke, c], preferred_element_type=jnp.float32)
                logit[j, :, i * cw : (i + 1) * cw] = l
                for n in range(0, cw, 128):
                    new = jnp.maximum(new, l[:, n : n + 128])
                low = l.astype(jnp.bfloat16)
                base = (v * G + m * a + ke) * cols + c * cw
                ids = lax.broadcasted_iota(jnp.int32, (cw, slots), 0) + base
                for q in range(unit):
                    hot = (ids == lg[g, pr * unit + q]).astype(jnp.float32).astype(jnp.bfloat16)
                    got = jnp.dot(low[q * frames : (q + 1) * frames], hot, preferred_element_type=jnp.float32)
                    acc[p, q] = acc[p, q] + got
            s = sm[p] * jnp.exp(old - new)
            for n in range(0, len(es) * cw, 128):
                s = s + jnp.exp(logit[j, :, n : n + 128] - new)
            mx[p] = new
            sm[p] = s

    def clear(p, _):
        mx[p] = jnp.full((rows, 128), LOW, jnp.float32)
        sm[p] = jnp.zeros((rows, 128), jnp.float32)
        acc[p] = jnp.zeros((unit, frames, slots), jnp.float32)
        return 0

    def chunks_of(d, h, count):
        lax.fori_loop(0, count // 2, lambda i, _: (task([(d, h)], [2 * i, 2 * i + 1]), 0)[1], 0)
        if count % 2:
            task([(d, h)], [count - 1])

    def pairs_of(count, e):
        at = lambda i: (turn(i // half), i % half)
        lax.fori_loop(0, count // 2, lambda i, _: (task([at(2 * i), at(2 * i + 1)], [e]), 0)[1], 0)
        if count % 2:
            task([at(count - 1)], [e])

    for c in local[2:]:
        c.wait()
    lax.fori_loop(0, pairs, clear, 0)

    events = []
    for t in range(1, b):
        events.append((0.2 * max(t - 1, 1), 0, t, 0))
        events.append((0.2 * t, 1, t, 0))
        for h in range(half):
            events.append((0.2 * t + 0.03 + 0.17 * h, 2, t, h))
    for e in range(nc, chunks - 1):
        events.append(((e - nc + 1) / (chunks - nc), 3, e, 0))
    events.sort()

    lax.fori_loop(0, half, lambda h, _: (chunks_of(0, h, nc), 0)[1], 0)
    have_p, have_e = half, nc
    for _, kind, i, h in events:
        if kind == 0:
            pl.when(inner)(functools.partial(recv_line, i))
        elif kind == 1:
            pl.when(jnp.logical_not(inner))(functools.partial(recv_line, i))
        elif kind == 2:
            if h > 0:
                recv_side(i, 2 * h)
            recv_side(i, 2 * h + 1)
            chunks_of(turn(i), h, have_e)
            have_p += 1
        else:
            recv_chunk(i)
            pairs_of(have_p, i)
            have_e = i + 1

    lane = lax.broadcasted_iota(jnp.int32, (frames, 128), 1)
    tall = 4 * unit

    def merge(p, q):
        odd = lax.broadcasted_iota(jnp.int32, (tall, frames), 0) % 2 == 1
        pt, qt = pltpu.roll(p, 1, 0), pltpu.roll(q, 1, 0)
        top = jnp.maximum(pt, qt)
        total = p * jnp.exp(pt - top) + q * jnp.exp(qt - top)
        return jnp.where(odd, total, jnp.maximum(p, q))

    def finish(n, which):
        tile = jnp.zeros((frames, 128), jnp.float32)
        for j, (d, h) in enumerate(which):
            p = d * half + h
            best = mx[p]
            top = jnp.max(best, 1, keepdims=True)
            total = jnp.sum(sm[p] * jnp.exp(best - top), 1, keepdims=True)
            for q in range(unit):
                part = slice(q * frames, (q + 1) * frames)
                pp[p, q // own, q % own] = acc[p, q].astype(jnp.bfloat16)
                at = 2 * (j * unit + q)
                tile = jnp.where(lane == at, top[part], tile)
                tile = jnp.where(lane == at + 1, total[part], tile)
        st[n] = tile.T[:tall]
        for d, h in which:
            p = d * half + h
            launch(pp.at[p, 1 - side], pin.at[p], sp.at[p], rp.at[p], sibling)
        launch(st.at[n], sin.at[n], ss.at[n], rs.at[n], sibling)

    def join_sibling(n, which):
        for d, h in which:
            p = d * half + h
            remote(pin.at[p], pin.at[p], sp.at[p], rp.at[p], sibling).wait_recv()
            cs[p] = pp[p, side] + pin[p]
            if h:
                launch(cs.at[p], xin.at[d, h - 1], sq.at[p], rq.at[d, h - 1], across(h))
        remote(sin.at[n], sin.at[n], ss.at[n], rs.at[n], sibling).wait_recv()
        cst[n] = merge(st[n], sin[n])
        h = which[0][1]
        if h:
            t = which[0][0] // 2
            launch(cst.at[n], xst.at[t, h - 1], sv.at[n], rv.at[t, h - 1], across(h))

    def join_across(n, which):
        t = which[0][0] // 2
        for d, _ in which:
            total = cs[d * half]
            for h in range(1, half):
                remote(xin.at[d, h - 1], xin.at[d, h - 1], sq.at[0], rq.at[d, h - 1], across(h)).wait_recv()
                total = total + xin[d, h - 1]
            if d:
                xout[d] = total
                launch(xout.at[d], zin.at[d], sz.at[d], rz.at[d], row_peer(d))
            else:
                zin[d] = total
        tile = cst[n]
        for h in range(1, half):
            remote(xst.at[t, h - 1], xst.at[t, h - 1], sv.at[0], rv.at[t, h - 1], across(h)).wait_recv()
            tile = merge(tile, xst[t, h - 1])
        zsrc[t] = tile
        for d, _ in which:
            if d:
                launch(zsrc.at[t], zst.at[d], sy.at[d], ry.at[d], row_peer(d))
            else:
                zst[d] = tile

    for c in sent[: (a - 1) * (nc - 1)]:
        c.wait_send()
    del sent[: (a - 1) * (nc - 1)]
    for t in range(1, b):
        o = jnp.bitwise_xor(m, turn(t))
        for mask in range(1, V):
            src = piece(o, v)
            remote(src, src, sx.at[t, mask], rf.at[o, mask], across(0)).wait_send()
    for o in range(b):
        src, tag = piece(o, v), lg.at[o]
        for i, go in enumerate(((o <= m) & (m < b - 1), (o >= m) & (m > 0))):
            pl.when(go)(remote(src, src, su.at[o, i], rf.at[o, 0], across(0)).wait_send)
            pl.when(go)(remote(tag, tag, sl.at[o, i], rl.at[o], across(0)).wait_send)
    recv_chunk(chunks - 1)
    blocks = [[(2 * t + 1, h), (2 * t, h)] for h in reversed(range(half)) for t in reversed(range(b // 2))]
    for n, which in enumerate(blocks):
        task(which, [chunks - 1])
        finish(n, which)
        if n:
            join_sibling(n - 1, blocks[n - 1])
    last = len(blocks) - 1
    join_sibling(last, blocks[last])
    for n, which in enumerate(blocks):
        if which[0][1] == 0:
            join_across(n, which)

    for q in range(own):
        got = zin[0, q]
        for d in range(1, b):
            if q == 0:
                remote(zin.at[d], zin.at[d], sz.at[d], rz.at[d], row_peer(d)).wait_recv()
                remote(zst.at[d], zst.at[d], sy.at[d], ry.at[d], row_peer(d)).wait_recv()
            got = got + zin[d, q]
        tops, sums = [], []
        for d in range(b):
            at = 2 * ((1 - d % 2) * unit + side * own + q)
            tops.append(zst[d, pl.ds(at, 1), :])
            sums.append(zst[d, pl.ds(at + 1, 1), :])
        top = tops[0]
        for one in tops[1:]:
            top = jnp.maximum(top, one)
        total = jnp.zeros_like(top)
        for one, part in zip(tops, sums):
            total = total + part * jnp.exp(one - top)
        pick_ref[q] = got
        stat_ref[q] = jnp.broadcast_to(top + jnp.log(total), (8, frames))

    for c in sent:
        c.wait_send()


def align_kernel(alen, tlen, pick, stat, lp_ref, out_ref, right, left):
    own, frames, slots = pick.shape
    lane = lax.broadcasted_iota(jnp.int32, (1, own), 1)
    scores = jnp.zeros((1, own), jnp.float32)
    for q in range(own):
        norm = jnp.broadcast_to(stat[q, 0:1, :], (slots, frames)).T
        lp_ref[q] = pick[q].astype(jnp.float32) - norm
        last, goal = alen[0:1, q : q + 1] - 1, tlen[0:1, q : q + 1] - 1
        scores = jnp.where(lane == q, best_path(q, last, goal, lp_ref, right, left), scores)
    out_ref[...] = scores


def body(features, head_weight, labels, audio_len, transcript_len):
    rec_dev, frames, width = features.shape
    cols = head_weight.shape[1]
    slots = labels.shape[1]
    G, V = lax.axis_size("rec"), lax.axis_size("vocab")
    best = None
    a = 2
    while a < G:
        cost = (a - 1) * width * cols + (G // a - 1) * features.size
        if G % a == 0 and (best is None or cost < best[0]):
            best = (cost, a)
        a *= 2
    a = best[1]
    b = G // a
    own = rec_dev // V
    vmem = pl.BlockSpec(memory_space=pltpu.VMEM)
    hbm = pl.BlockSpec(memory_space=pl.ANY)
    dma = pltpu.SemaphoreType.DMA
    cw = min(256, cols)
    nc = cols // cw
    unit = 2 * own
    pairs = b * (V // 2)
    rows = unit * frames
    bf, f32 = jnp.bfloat16, jnp.float32
    half = V // 2
    tall = 4 * unit
    one = (own, frames, slots)
    pick, stat = pl.pallas_call(
        functools.partial(emit_kernel, a, b, V),
        out_shape=(jax.ShapeDtypeStruct(one, bf), jax.ShapeDtypeStruct((own, 8, frames), f32)),
        in_specs=[hbm] * 3,
        out_specs=(vmem, vmem),
        scratch_shapes=[
            pltpu.VMEM((b,) + features.shape, features.dtype),
            pltpu.VMEM((a, nc, width, cw), head_weight.dtype),
            pltpu.VMEM((b, rec_dev, 1, slots), jnp.int32),
            pltpu.VMEM((pairs, rows, 128), f32),
            pltpu.VMEM((pairs, rows, 128), f32),
            pltpu.VMEM((pairs, unit, frames, slots), f32),
            pltpu.VMEM((2, rows, 2 * cw), f32),
            pltpu.VMEM((pairs, 2) + one, bf),
            pltpu.VMEM((pairs,) + one, bf),
            pltpu.VMEM((pairs,) + one, bf),
            pltpu.VMEM((b, half - 1) + one, bf),
            pltpu.VMEM((b,) + one, bf),
            pltpu.VMEM((b,) + one, bf),
            pltpu.VMEM((pairs // 2, tall, frames), f32),
            pltpu.VMEM((pairs // 2, tall, frames), f32),
            pltpu.VMEM((pairs // 2, tall, frames), f32),
            pltpu.VMEM((b // 2, half - 1, tall, frames), f32),
            pltpu.VMEM((b // 2, tall, frames), f32),
            pltpu.VMEM((b, tall, frames), f32),
            dma((a - 1, nc)), dma((a - 1, nc)), dma((b, 2)), dma((b,)),
            dma((b, 2)), dma((b, V)), dma((b, V)),
            dma((pairs,)), dma((pairs,)), dma((pairs // 2,)), dma((pairs // 2,)),
            dma((pairs,)), dma((b, half - 1)), dma((pairs // 2,)), dma((b // 2, half - 1)),
            dma((b,)), dma((b,)), dma((b,)), dma((b,)), dma((2 + nc,)),
        ],
        compiler_params=pltpu.CompilerParams(
            collective_id=0, has_side_effects=True, vmem_limit_bytes=54700 * 1024
        ),
        name="emit",
    )(features, head_weight, labels.reshape(rec_dev, 1, slots))

    log_prob, score = pl.pallas_call(
        align_kernel,
        out_shape=(jax.ShapeDtypeStruct(one, f32), jax.ShapeDtypeStruct((1, own), f32)),
        in_specs=[vmem] * 4,
        out_specs=(vmem, vmem),
        scratch_shapes=[pltpu.VMEM((run - 1, frames, slots), f32), pltpu.VMEM((run, frames, slots), f32)],
        compiler_params=pltpu.CompilerParams(vmem_limit_bytes=8 * 1024 * 1024),
        name="align",
    )(audio_len.reshape(1, own), transcript_len.reshape(1, own), pick, stat)
    return log_prob, score.reshape(own)


def solution(mesh):
    return jax.shard_map(
        body,
        mesh=mesh,
        in_specs=(
            P("rec", None, None),
            P(None, ("vocab", "rec")),
            P("rec", None),
            P(("rec", "vocab")),
            P(("rec", "vocab")),
        ),
        out_specs=(P(("rec", "vocab"), None, None), P(("rec", "vocab"))),
        check_vma=False,
    )
```

```python
import functools
import jax
import jax.numpy as jnp
from jax import lax
from jax.experimental import pallas as pl
from jax.experimental.pallas import tpu as pltpu
from jax.sharding import PartitionSpec as P

MESH = pl.DeviceIdType.MESH
NEG = -1e30
LOW = -3e38
run = 8


def bits_of(size):
    bits = []
    bit = size // 2
    while bit >= 1:
        bits.append(bit)
        bit //= 2
    return bits


def flip(v, mask, size):
    for bit in bits_of(size):
        if mask & bit:
            v = v + bit * (1 - 2 * ((v // bit) % 2))
    return v


def best_path(q, last, goal, lp_ref, right, left):
    own, frames, slots = lp_ref.shape
    lane = lax.broadcasted_iota(jnp.int32, (1, slots), 1)
    whole = lp_ref[q]
    for c in range(1, run):
        right[c - 1] = pltpu.roll(whole, c, 1)
    for c in range(1, run + 1):
        left[c - 1] = pltpu.roll(whole, slots - c, 1)
    mid = frames // 2

    def row(shifted, c, t):
        return lp_ref[q, pl.ds(t, 1), :] if c == 0 else shifted[c - 1, pl.ds(t, 1), :]

    def forward(t, steps, cur, best):
        moved = [cur] + [jnp.where(lane < c, NEG, pltpu.roll(cur, c, 1)) for c in range(1, steps + 1)]
        for i in range(steps):
            moved = [jnp.maximum(moved[c], moved[c + 1]) + row(right, c, t + i) for c in range(steps - i)]
            best = jnp.where(last == t + i, moved[0], best)
        return moved[0], best

    ends = [jnp.where(lane + c == goal, 0.0, NEG) for c in range(run + 1)]

    def backward(t, steps, cur):
        moved = [cur] + [jnp.where(lane >= slots - c, NEG, pltpu.roll(cur, slots - c, 1)) for c in range(1, steps + 1)]
        for i in range(steps):
            moved = [jnp.where(last == t - i, ends[c], moved[c]) + row(left, c, t - i) for c in range(steps - i + 1)]
            moved = [jnp.maximum(moved[c], moved[c + 1]) for c in range(steps - i)]
        return moved[0]

    first = jnp.where(lane == 0, lp_ref[q, 0:1, :], NEG)
    ahead, behind = mid - 1, frames - mid
    count = min(ahead, behind) // run

    def both(i, carry):
        cur, best, tail = carry
        cur, best = forward(1 + i * run, run, cur, best)
        return cur, best, backward(frames - 1 - i * run, run, tail)

    cur, best, tail = lax.fori_loop(0, count, both, (first, first, jnp.full((1, slots), NEG, jnp.float32)))
    done = count * run
    at = done
    while at < ahead:
        cur, best = forward(1 + at, min(run, ahead - at), cur, best)
        at += min(run, ahead - at)
    at = done
    while at < behind:
        tail = backward(frames - 1 - at, min(run, behind - at), tail)
        at += min(run, behind - at)
    early = jnp.sum(jnp.where(lane == goal, best, 0.0), 1, keepdims=True)
    late = jnp.max(cur + tail, 1, keepdims=True)
    return jnp.where(last < mid, early, late)


def emit_kernel(
    a, b, V, x, w, lab, pick_ref, stat_ref, xg, wg, lg, mx, sm, acc, logit,
    pp, pin, cs, xin, xout, zin, st, sin, cst, xst, zsrc, zst,
    sw, rw, sl, rl, su, sx, rf, sp, rp, ss, rs, sq, rq, sv, rv, sz, rz, sy, ry, loc,
):
    r = lax.axis_index("rec")
    v = lax.axis_index("vocab")
    G = a * b
    m, k = r // a, r % a
    rec_dev, frames, width = x.shape
    own = rec_dev // V
    nc, cw = wg.shape[1], wg.shape[3]
    cols = nc * cw
    slots = lab.shape[2]
    half = V // 2
    side = v % 2
    bits = bits_of(V)
    unit = 2 * own
    rows = unit * frames
    pairs = b * half
    chunks = a * nc

    def among(values, i):
        out = values[0]
        for j in range(1, len(values)):
            out = jnp.where(i == j, values[j], out)
        return out

    near = [sorted(range(b), key=lambda o: (abs(o - i), o)) for i in range(b)]
    turns = [among([near[i][t] ^ i for i in range(b)], m) for t in range(b)]
    turn = lambda t: turns[t] if isinstance(t, int) else among(turns, t)
    inner = (m > 0) & (m < b - 1)

    col_peer = lambda d: (m * a + flip(k, d, a), v)
    row_peer = lambda d: (flip(m, d, b) * a + k, v)
    line = lambda at: (at * a + k, v)
    sibling = (r, flip(v, 1, V))
    across = lambda h: (r, flip(v, 2 * h, V))

    local = [pltpu.make_async_copy(x, xg.at[m], loc.at[0]), pltpu.make_async_copy(lab, lg.at[m], loc.at[1])]
    for c in range(nc):
        local.append(pltpu.make_async_copy(w.at[:, pl.ds(c * cw, cw)], wg.at[k, c], loc.at[2 + c]))
    for c in local:
        c.start()

    barrier = pltpu.get_barrier_semaphore()
    peers = [col_peer(d) for d in range(1, a)]
    peers += [(r, flip(v, mask, V)) for mask in sorted(set(bits + [2 * h for h in range(1, half)]))]

    def greet(peer):
        pl.semaphore_signal(barrier, inc=1, device_id=peer, device_id_type=MESH)

    for peer in peers:
        greet(peer)
    pl.when(m < b - 1)(lambda: greet(line(m + 1)))
    pl.when(m > 0)(lambda: greet(line(m - 1)))
    pl.semaphore_wait(barrier, len(peers) + jnp.minimum(m, 1) + jnp.minimum(b - 1 - m, 1))

    def remote(src, dst, s, t, to):
        return pltpu.make_async_remote_copy(
            src_ref=src, dst_ref=dst, send_sem=s, recv_sem=t, device_id=to, device_id_type=MESH
        )

    sent = []

    def launch(*args):
        c = remote(*args)
        c.start()
        sent.append(c)

    piece = lambda g, c: xg.at[g, pl.ds(c * own, own)]
    for c in range(nc):
        for d in range(1, a):
            ref = wg.at[k, c]
            launch(w.at[:, pl.ds(c * cw, cw)], ref, sw.at[d - 1, c], rw.at[d - 1, c], col_peer(d))
    def pass_on(o, up, go):
        src = piece(o, v)
        to = line(m + 1 if up else m - 1)
        c = remote(src, src, su.at[o, 0 if up else 1], rf.at[o, 0], to)
        tags = remote(lg.at[o], lg.at[o], sl.at[o, 0 if up else 1], rl.at[o], to)

        def start():
            tags.start()
            c.start()

        pl.when(go)(start)

    local[0].wait()
    local[1].wait()
    pass_on(m, True, m < b - 1)
    pass_on(m, False, m > 0)

    def recv_line(t):
        o = jnp.bitwise_xor(m, turn(t))
        src = piece(o, v)
        remote(lg.at[o], lg.at[o], sl.at[o, 0], rl.at[o], across(0)).wait_recv()
        remote(src, src, sx.at[t, 0], rf.at[o, 0], across(0)).wait_recv()
        pass_on(o, True, (o < m) & (m < b - 1))
        pass_on(o, False, (o > m) & (m > 0))
        for bit in bits:
            remote(src, src, sx.at[t, bit], rf.at[o, bit], (r, flip(v, bit, V))).start()

    def recv_side(t, mask):
        o = jnp.bitwise_xor(m, turn(t))
        low = mask & -mask
        src = piece(o, flip(v, mask, V))
        remote(src, src, sx.at[t, mask], rf.at[o, mask], across(0)).wait_recv()
        for bit in bits:
            if bit < low:
                remote(src, src, sx.at[t, mask | bit], rf.at[o, mask | bit], (r, flip(v, bit, V))).start()

    def recv_chunk(e):
        d, c = e // nc, e % nc
        ref = wg.at[flip(k, d, a), c]
        remote(ref, ref, sw.at[d - 1, c], rw.at[d - 1, c], col_peer(d)).wait_recv()

    def task(which, es):
        for j, (d, h) in enumerate(which):
            p = d * half + h
            g, pr = jnp.bitwise_xor(m, d), jnp.bitwise_xor(v // 2, h)
            xs = xg[g, pl.ds(pr * unit, unit)].reshape(rows, width)
            old = mx[p]
            new = old
            base = []
            for i, e in enumerate(es):
                ke = jnp.bitwise_xor(k, e // nc)
                c = e % nc
                l = jnp.dot(xs, wg[ke, c], preferred_element_type=jnp.float32)
                logit[j, :, i * cw : (i + 1) * cw] = l
                for n in range(0, cw, 128):
                    new = jnp.maximum(new, l[:, n : n + 128])
                low = l.astype(jnp.bfloat16)
                base = (v * G + m * a + ke) * cols + c * cw
                ids = lax.broadcasted_iota(jnp.int32, (cw, slots), 0) + base
                for q in range(unit):
                    hot = (ids == lg[g, pr * unit + q]).astype(jnp.float32).astype(jnp.bfloat16)
                    got = jnp.dot(low[q * frames : (q + 1) * frames], hot, preferred_element_type=jnp.float32)
                    acc[p, q] = acc[p, q] + got
            s = sm[p] * jnp.exp(old - new)
            for n in range(0, len(es) * cw, 128):
                s = s + jnp.exp(logit[j, :, n : n + 128] - new)
            mx[p] = new
            sm[p] = s

    def clear(p, _):
        mx[p] = jnp.full((rows, 128), LOW, jnp.float32)
        sm[p] = jnp.zeros((rows, 128), jnp.float32)
        acc[p] = jnp.zeros((unit, frames, slots), jnp.float32)
        return 0

    def chunks_of(d, h, count):
        lax.fori_loop(0, count // 2, lambda i, _: (task([(d, h)], [2 * i, 2 * i + 1]), 0)[1], 0)
        if count % 2:
            task([(d, h)], [count - 1])

    def pairs_of(count, e):
        at = lambda i: (turn(i // half), i % half)
        lax.fori_loop(0, count // 2, lambda i, _: (task([at(2 * i), at(2 * i + 1)], [e]), 0)[1], 0)
        if count % 2:
            task([at(count - 1)], [e])

    for c in local[2:]:
        c.wait()
    lax.fori_loop(0, pairs, clear, 0)

    events = []
    for t in range(1, b):
        events.append((0.2 * max(t - 1, 1), 0, t, 0))
        events.append((0.2 * t, 1, t, 0))
        for h in range(half):
            events.append((0.2 * t + 0.03 + 0.17 * h, 2, t, h))
    for e in range(nc, chunks - 1):
        events.append(((e - nc + 1) / (chunks - nc), 3, e, 0))
    events.sort()

    lax.fori_loop(0, half, lambda h, _: (chunks_of(0, h, nc), 0)[1], 0)
    have_p, have_e = half, nc
    for _, kind, i, h in events:
        if kind == 0:
            pl.when(inner)(functools.partial(recv_line, i))
        elif kind == 1:
            pl.when(jnp.logical_not(inner))(functools.partial(recv_line, i))
        elif kind == 2:
            if h > 0:
                recv_side(i, 2 * h)
            recv_side(i, 2 * h + 1)
            chunks_of(turn(i), h, have_e)
            have_p += 1
        else:
            recv_chunk(i)
            pairs_of(have_p, i)
            have_e = i + 1

    lane = lax.broadcasted_iota(jnp.int32, (frames, 128), 1)
    tall = 4 * unit

    def merge(p, q):
        odd = lax.broadcasted_iota(jnp.int32, (tall, frames), 0) % 2 == 1
        pt, qt = pltpu.roll(p, 1, 0), pltpu.roll(q, 1, 0)
        top = jnp.maximum(pt, qt)
        total = p * jnp.exp(pt - top) + q * jnp.exp(qt - top)
        return jnp.where(odd, total, jnp.maximum(p, q))

    many = b // 2
    span_of = lambda which: pl.ds(which[1][0], 2)

    def finish(n, which):
        tile = jnp.zeros((frames, 128), jnp.float32)
        for j, (d, h) in enumerate(which):
            p = d * half + h
            best = mx[p]
            top = jnp.max(best, 1, keepdims=True)
            total = jnp.sum(sm[p] * jnp.exp(best - top), 1, keepdims=True)
            for q in range(unit):
                part = slice(q * frames, (q + 1) * frames)
                pp[q // own, h, d, q % own] = acc[p, q].astype(jnp.bfloat16)
                at = 2 * (j * unit + q)
                tile = jnp.where(lane == at, top[part], tile)
                tile = jnp.where(lane == at + 1, total[part], tile)
        st[n] = tile.T[:tall]
        h, span = which[0][1], span_of(which)
        launch(pp.at[1 - side, h, span], pin.at[h, span], sp.at[n], rp.at[n], sibling)
        if n % many == many - 1:
            group = pl.ds(n + 1 - many, many)
            launch(st.at[group], sin.at[group], ss.at[h], rs.at[h], sibling)

    def join_picks(n, which):
        h, span = which[0][1], span_of(which)
        remote(pin.at[h, span], pin.at[h, span], sp.at[n], rp.at[n], sibling).wait_recv()
        cs[h, span] = pp[side, h, span] + pin[h, span]
        if h:
            launch(cs.at[h, span], xin.at[h - 1, span], sq.at[n], rq.at[h - 1, n % many], across(h))

    def join_sums(h):
        first = (half - 1 - h) * many
        group = pl.ds(first, many)
        remote(st.at[group], sin.at[group], ss.at[h], rs.at[h], sibling).wait_recv()
        for n in range(first, first + many):
            cst[n] = merge(st[n], sin[n])
        if h:
            launch(cst.at[group], xst.at[h - 1], sv.at[h], rv.at[h - 1], across(h))

    def across_picks(n, which):
        span = span_of(which)
        for h in range(1, half):
            ref = xin.at[h - 1, span]
            remote(ref, ref, sq.at[0], rq.at[h - 1, n % many], across(h)).wait_recv()
        for d, _ in which:
            total = cs[0, d]
            for h in range(1, half):
                total = total + xin[h - 1, d]
            if d:
                xout[d] = total
                launch(xout.at[d], zin.at[d], sz.at[d], rz.at[d], row_peer(d))
            else:
                zin[d] = total

    def across_sums():
        for h in range(1, half):
            remote(xst.at[h - 1], xst.at[h - 1], sv.at[h], rv.at[h - 1], across(h)).wait_recv()
        for n, which in enumerate(blocks):
            if which[0][1]:
                continue
            tile = cst[n]
            for h in range(1, half):
                tile = merge(tile, xst[h - 1, n % many])
            t = which[1][0] // 2
            zsrc[t] = tile
            for d, _ in which:
                if d:
                    launch(zsrc.at[t], zst.at[d], sy.at[d], ry.at[d], row_peer(d))
                else:
                    zst[d] = tile

    for c in sent[: (a - 1) * (nc - 1)]:
        c.wait_send()
    del sent[: (a - 1) * (nc - 1)]
    for t in range(1, b):
        o = jnp.bitwise_xor(m, turn(t))
        for mask in range(1, V):
            src = piece(o, v)
            remote(src, src, sx.at[t, mask], rf.at[o, mask], across(0)).wait_send()
    for o in range(b):
        src, tag = piece(o, v), lg.at[o]
        for i, go in enumerate(((o <= m) & (m < b - 1), (o >= m) & (m > 0))):
            pl.when(go)(remote(src, src, su.at[o, i], rf.at[o, 0], across(0)).wait_send)
            pl.when(go)(remote(tag, tag, sl.at[o, i], rl.at[o], across(0)).wait_send)
    recv_chunk(chunks - 1)
    blocks = [[(2 * t + 1, h), (2 * t, h)] for h in reversed(range(half)) for t in reversed(range(many))]
    last = len(blocks) - 1
    for n, which in enumerate(blocks):
        task(which, [chunks - 1])
        finish(n, which)
        if n:
            join_picks(n - 1, blocks[n - 1])
        if n and n % many == 0:
            join_sums(blocks[n - 1][0][1])
    join_picks(last, blocks[last])
    home = [n for n in range(last + 1) if blocks[n][0][1] == 0]
    across_picks(home[0], blocks[home[0]])
    join_sums(0)
    across_sums()
    for n in home[1:]:
        across_picks(n, blocks[n])

    for q in range(own):
        got = zin[0, q]
        for d in range(1, b):
            if q == 0:
                remote(zin.at[d], zin.at[d], sz.at[d], rz.at[d], row_peer(d)).wait_recv()
                remote(zst.at[d], zst.at[d], sy.at[d], ry.at[d], row_peer(d)).wait_recv()
            got = got + zin[d, q]
        tops, sums = [], []
        for d in range(b):
            at = 2 * ((1 - d % 2) * unit + side * own + q)
            tops.append(zst[d, pl.ds(at, 1), :])
            sums.append(zst[d, pl.ds(at + 1, 1), :])
        top = tops[0]
        for one in tops[1:]:
            top = jnp.maximum(top, one)
        total = jnp.zeros_like(top)
        for one, part in zip(tops, sums):
            total = total + part * jnp.exp(one - top)
        pick_ref[q] = got
        stat_ref[q] = jnp.broadcast_to(top + jnp.log(total), (8, frames))

    for c in sent:
        c.wait_send()


def align_kernel(alen, tlen, pick, stat, lp_ref, out_ref, right, left):
    own, frames, slots = pick.shape
    lane = lax.broadcasted_iota(jnp.int32, (1, own), 1)
    scores = jnp.zeros((1, own), jnp.float32)
    for q in range(own):
        norm = jnp.broadcast_to(stat[q, 0:1, :], (slots, frames)).T
        lp_ref[q] = pick[q].astype(jnp.float32) - norm
        last, goal = alen[0:1, q : q + 1] - 1, tlen[0:1, q : q + 1] - 1
        scores = jnp.where(lane == q, best_path(q, last, goal, lp_ref, right, left), scores)
    out_ref[...] = scores


def body(features, head_weight, labels, audio_len, transcript_len):
    rec_dev, frames, width = features.shape
    cols = head_weight.shape[1]
    slots = labels.shape[1]
    G, V = lax.axis_size("rec"), lax.axis_size("vocab")
    best = None
    a = 2
    while a < G:
        cost = (a - 1) * width * cols + (G // a - 1) * features.size
        if G % a == 0 and (best is None or cost < best[0]):
            best = (cost, a)
        a *= 2
    a = best[1]
    b = G // a
    own = rec_dev // V
    vmem = pl.BlockSpec(memory_space=pltpu.VMEM)
    hbm = pl.BlockSpec(memory_space=pl.ANY)
    dma = pltpu.SemaphoreType.DMA
    cw = min(256, cols)
    nc = cols // cw
    unit = 2 * own
    pairs = b * (V // 2)
    rows = unit * frames
    bf, f32 = jnp.bfloat16, jnp.float32
    half = V // 2
    tall = 4 * unit
    one = (own, frames, slots)
    pick, stat = pl.pallas_call(
        functools.partial(emit_kernel, a, b, V),
        out_shape=(jax.ShapeDtypeStruct(one, bf), jax.ShapeDtypeStruct((own, 8, frames), f32)),
        in_specs=[hbm] * 3,
        out_specs=(vmem, vmem),
        scratch_shapes=[
            pltpu.VMEM((b,) + features.shape, features.dtype),
            pltpu.VMEM((a, nc, width, cw), head_weight.dtype),
            pltpu.VMEM((b, rec_dev, 1, slots), jnp.int32),
            pltpu.VMEM((pairs, rows, 128), f32),
            pltpu.VMEM((pairs, rows, 128), f32),
            pltpu.VMEM((pairs, unit, frames, slots), f32),
            pltpu.VMEM((2, rows, 2 * cw), f32),
            pltpu.VMEM((2, half, b) + one, bf),
            pltpu.VMEM((half, b) + one, bf),
            pltpu.VMEM((half, b) + one, bf),
            pltpu.VMEM((half - 1, b) + one, bf),
            pltpu.VMEM((b,) + one, bf),
            pltpu.VMEM((b,) + one, bf),
            pltpu.VMEM((pairs // 2, tall, frames), f32),
            pltpu.VMEM((pairs // 2, tall, frames), f32),
            pltpu.VMEM((pairs // 2, tall, frames), f32),
            pltpu.VMEM((half - 1, b // 2, tall, frames), f32),
            pltpu.VMEM((b // 2, tall, frames), f32),
            pltpu.VMEM((b, tall, frames), f32),
            dma((a - 1, nc)), dma((a - 1, nc)), dma((b, 2)), dma((b,)),
            dma((b, 2)), dma((b, V)), dma((b, V)),
            dma((pairs // 2,)), dma((pairs // 2,)), dma((half,)), dma((half,)),
            dma((pairs // 2,)), dma((half - 1, b // 2)), dma((half,)), dma((half - 1,)),
            dma((b,)), dma((b,)), dma((b,)), dma((b,)), dma((2 + nc,)),
        ],
        compiler_params=pltpu.CompilerParams(
            collective_id=0, has_side_effects=True, vmem_limit_bytes=54700 * 1024
        ),
        name="emit",
    )(features, head_weight, labels.reshape(rec_dev, 1, slots))

    log_prob, score = pl.pallas_call(
        align_kernel,
        out_shape=(jax.ShapeDtypeStruct(one, f32), jax.ShapeDtypeStruct((1, own), f32)),
        in_specs=[vmem] * 4,
        out_specs=(vmem, vmem),
        scratch_shapes=[pltpu.VMEM((run - 1, frames, slots), f32), pltpu.VMEM((run, frames, slots), f32)],
        compiler_params=pltpu.CompilerParams(vmem_limit_bytes=8 * 1024 * 1024),
        name="align",
    )(audio_len.reshape(1, own), transcript_len.reshape(1, own), pick, stat)
    return log_prob, score.reshape(own)


def solution(mesh):
    return jax.shard_map(
        body,
        mesh=mesh,
        in_specs=(
            P("rec", None, None),
            P(None, ("vocab", "rec")),
            P("rec", None),
            P(("rec", "vocab")),
            P(("rec", "vocab")),
        ),
        out_specs=(P(("rec", "vocab"), None, None), P(("rec", "vocab"))),
        check_vma=False,
    )
```
